128 devices in a mesh: rep: 1, tp: 16 (over z, y), ep: 8 (over x, core).
Axes of the slice: x: 4, y: 4, z: 4, core: 2. Of those that a mesh axis runs over, the one named last changes fastest.
Arguments:
- x_in: bfloat16 [8192, 1536], P(('rep', 'ep'))
- route_ids: int32 [2, 8192, 8], P(None, ('rep', 'ep'))
- gate_vals: float32 [2, 8192, 8], P(None, ('rep', 'ep'))
- w_gate: bfloat16 [2, 64, 1536, 512], P(None, ('rep', 'ep'), None, 'tp')
- w_up: bfloat16 [2, 64, 1536, 512], P(None, ('rep', 'ep'), None, 'tp')
- w_down: bfloat16 [2, 64, 512, 1536], P(None, ('rep', 'ep'), 'tp')
- old_map: int32 [2, 64], replicated
- move_src: int32 [2, 32], replicated
- move_dst: int32 [2, 32], replicated
Outputs:
- output 1: bfloat16 [8192, 1536], P(('rep', 'ep'))
- output 2: bfloat16 [2, 64, 1536, 512], P(None, ('rep', 'ep'), None, 'tp')
- output 3: bfloat16 [2, 64, 1536, 512], P(None, ('rep', 'ep'), None, 'tp')
- output 4: bfloat16 [2, 64, 512, 1536], P(None, ('rep', 'ep'), 'tp')
All inputs are finite; a program needn't handle non-finite values.
Results may differ from the reference program's by a relative error of at most 0.0073047.
Values are sent between devices in bfloat16 or wider.
A program may use at most 1 GiB of HBM per device.

```python
import jax
import jax.numpy as jnp
from jax import lax

MODEL_DIM = 1536
FFN_DIM = 512
EXPERTS = 40
TOP_K = 8
LOCAL_SLOTS = 8
TOKENS_DEV = 1024
NUM_MOVES = 32
GROUP_SIZE = 8
NUM_LAYERS = 2

NUM_SLOTS = GROUP_SIZE * LOCAL_SLOTS
GROUP_TOKENS = GROUP_SIZE * TOKENS_DEV
CAPACITY = 2 * TOKENS_DEV * TOP_K // NUM_SLOTS
EXPERT_ROWS = GROUP_SIZE * CAPACITY


def device_routes(rng_key):
    hot_count = EXPERTS // 4
    rest_total = TOKENS_DEV * TOP_K - hot_count * CAPACITY
    rest_base = rest_total // (EXPERTS - hot_count)
    rest_extra = rest_total % (EXPERTS - hot_count)
    rank_ids = jnp.arange(EXPERTS, dtype=jnp.int32)
    counts = jnp.where(rank_ids < hot_count, CAPACITY, rest_base + (rank_ids - hot_count < rest_extra).astype(jnp.int32))
    key_label, key_token = jax.random.split(rng_key)
    labels = jax.random.permutation(key_label, EXPERTS).astype(jnp.int32)
    run_ends = jnp.cumsum(counts)
    entries = jnp.arange(TOKENS_DEV * TOP_K, dtype=jnp.int32)
    rank_of = jnp.searchsorted(run_ends, entries, side='right')
    expert_of = labels[rank_of].reshape(TOP_K, TOKENS_DEV).T
    token_order = jax.random.permutation(key_token, TOKENS_DEV)
    return expert_of[token_order]


def layer_maps(rng_key):
    key_extra, key_slot, key_move = jax.random.split(rng_key, 3)
    extra_ids = jax.random.randint(key_extra, (NUM_SLOTS - EXPERTS,), 0, EXPERTS, dtype=jnp.int32)
    slot_expert = jnp.concatenate([jnp.arange(EXPERTS, dtype=jnp.int32), extra_ids])
    slot_perm = jax.random.permutation(key_slot, NUM_SLOTS).astype(jnp.int32)
    old_map = jnp.zeros((NUM_SLOTS,), jnp.int32).at[slot_perm].set(slot_expert)
    chosen = jax.random.permutation(key_move, EXPERTS)[:NUM_MOVES].astype(jnp.int32)
    move_dst = slot_perm[chosen]
    move_src = slot_perm[jnp.roll(chosen, -1)]
    return old_map, move_src, move_dst


def setup_inputs(seed: int = 0, part: int = 0) -> dict:
    root_key = jax.random.key(seed)
    key_shared, key_group = jax.random.split(root_key)
    key_part = jax.random.fold_in(key_group, part)
    old_map, move_src, move_dst = jax.vmap(layer_maps)(jax.random.split(key_shared, NUM_LAYERS))
    key_x, key_route, key_gate, key_wg, key_wu, key_wd = jax.random.split(key_part, 6)
    x_in = jax.random.normal(key_x, (GROUP_TOKENS, MODEL_DIM), jnp.float32).astype(jnp.bfloat16)
    route_ids = jax.vmap(device_routes)(jax.random.split(key_route, NUM_LAYERS * GROUP_SIZE)).reshape(NUM_LAYERS, GROUP_TOKENS, TOP_K)
    gate_vals = jax.random.uniform(key_gate, (NUM_LAYERS, GROUP_TOKENS, TOP_K), jnp.float32, 0.5, 1.5) * TOP_K ** -0.5
    table_gate = (jax.random.normal(key_wg, (NUM_LAYERS, EXPERTS, MODEL_DIM, FFN_DIM), jnp.float32) * MODEL_DIM ** -0.5).astype(jnp.bfloat16)
    table_up = (jax.random.normal(key_wu, (NUM_LAYERS, EXPERTS, MODEL_DIM, FFN_DIM), jnp.float32) * MODEL_DIM ** -0.5).astype(jnp.bfloat16)
    table_down = (jax.random.normal(key_wd, (NUM_LAYERS, EXPERTS, FFN_DIM, MODEL_DIM), jnp.float32) * FFN_DIM ** -0.5).astype(jnp.bfloat16)
    place_slots = jax.vmap(lambda expert_table, slot_map: expert_table[slot_map])
    return {'x_in': x_in, 'route_ids': route_ids, 'gate_vals': gate_vals, 'w_gate': place_slots(table_gate, old_map), 'w_up': place_slots(table_up, old_map), 'w_down': place_slots(table_down, old_map), 'old_map': old_map, 'move_src': move_src, 'move_dst': move_dst}


def moe_layer(hidden, layer_ids, layer_gates, w_gate, w_up, w_down, slot_map):
    first_slot = jax.ops.segment_min(jnp.arange(NUM_SLOTS, dtype=jnp.int32), slot_map, num_segments=EXPERTS)
    flat_ids = layer_ids.reshape(-1)
    sort_order = jnp.argsort(flat_ids, stable=True)
    sorted_tok = (sort_order // TOP_K).astype(jnp.int32)
    sorted_gate = layer_gates.reshape(-1)[sort_order]
    counts = jnp.zeros((EXPERTS,), jnp.int32).at[flat_ids].add(1)
    starts = jnp.cumsum(counts) - counts
    pad_tok = jnp.concatenate([sorted_tok, jnp.zeros((EXPERT_ROWS,), jnp.int32)])
    pad_gate = jnp.concatenate([sorted_gate, jnp.zeros((EXPERT_ROWS,), jnp.float32)])
    row_ids = jnp.arange(EXPERT_ROWS)

    def expert_step(token_acc, expert):
        row_start = starts[expert]
        tok_rows = lax.dynamic_slice(pad_tok, (row_start,), (EXPERT_ROWS,))
        row_gate = jnp.where(row_ids < counts[expert], lax.dynamic_slice(pad_gate, (row_start,), (EXPERT_ROWS,)), 0.0)
        slot_idx = first_slot[expert]
        tok_in = hidden[tok_rows]
        gate_acc = jnp.dot(tok_in, w_gate[slot_idx], preferred_element_type=jnp.float32)
        up_acc = jnp.dot(tok_in, w_up[slot_idx], preferred_element_type=jnp.float32)
        hidden_act = (jax.nn.silu(gate_acc) * up_acc).astype(jnp.bfloat16)
        expert_out = jnp.dot(hidden_act, w_down[slot_idx], preferred_element_type=jnp.float32).astype(jnp.bfloat16)
        token_acc = token_acc.at[tok_rows].add(row_gate[:, None] * expert_out.astype(jnp.float32))
        return token_acc, expert

    token_acc = lax.scan(expert_step, jnp.zeros((GROUP_TOKENS, MODEL_DIM), jnp.float32), jnp.arange(EXPERTS))[0]
    return (hidden.astype(jnp.float32) + token_acc).astype(jnp.bfloat16)


def relocate(weights, move_src, move_dst):
    return jax.vmap(lambda layer_w, src_slot, dst_slot: layer_w.at[dst_slot].set(layer_w[src_slot]))(weights, move_src, move_dst)


def reference(x_in, route_ids, gate_vals, w_gate, w_up, w_down, old_map, move_src, move_dst):
    hidden = x_in
    for layer_idx in range(NUM_LAYERS):
        hidden = moe_layer(hidden, route_ids[layer_idx], gate_vals[layer_idx], w_gate[layer_idx], w_up[layer_idx], w_down[layer_idx], old_map[layer_idx])
    return (hidden, relocate(w_gate, move_src, move_dst), relocate(w_up, move_src, move_dst), relocate(w_down, move_src, move_dst))
```

```python
import functools

import jax
import jax.numpy as jnp
from jax import lax
from jax.experimental import pallas as pl
from jax.experimental.pallas import tpu as pltpu
from jax.sharding import PartitionSpec as P

EXPERTS = 40
F32 = jnp.float32
BF16 = jnp.bfloat16


def combine_kernel(cap, group, slots, first_ref, back_ref, rank_ref, gate_ref, res_ref, out_ref, acc_ref):
    tokens = rank_ref.shape[1]
    feats = out_ref.shape[0]
    acc_ref[...] = res_ref[...].astype(F32)
    row_iota = lax.broadcasted_iota(jnp.int32, (cap, tokens), 0)

    def step(expert, carry):
        slot = first_ref[expert]
        owner = slot // slots
        pair = 2 * (slot - owner * slots)
        rows = back_ref[pl.ds(pair, 2), owner].reshape(cap, feats)
        pick = (rank_ref[pl.ds(expert, 1), :] == row_iota).astype(BF16)
        chosen = lax.dot_general(rows, pick, (((0,), (0,)), ((), ())), preferred_element_type=F32)
        acc_ref[...] += gate_ref[pl.ds(expert, 1), :] * chosen
        return carry

    lax.fori_loop(0, EXPERTS, step, 0)
    out_ref[...] = acc_ref[...].astype(BF16)


def combine(first_slot, back, rank, gate, residual, cap, group, slots):
    feats, tokens = residual.shape
    return pl.pallas_call(
        functools.partial(combine_kernel, cap, group, slots),
        out_shape=jax.ShapeDtypeStruct((feats, tokens), BF16),
        in_specs=[pl.BlockSpec(memory_space=pltpu.SMEM)] + [pl.BlockSpec(memory_space=pltpu.VMEM)] * 4,
        out_specs=pl.BlockSpec(memory_space=pltpu.VMEM),
        scratch_shapes=[pltpu.VMEM((feats, tokens), F32)],
        cost_estimate=pl.CostEstimate(flops=2 * EXPERTS * cap * 256 * tokens, bytes_accessed=8 << 20, transcendentals=0),
    )(first_slot, back, rank, gate, residual)


def solution(mesh):
    group = mesh.shape['ep']
    cols = mesh.shape['tp']
    row_spec = P(('rep', 'ep'), None)
    layer_spec = P(None, ('rep', 'ep'), None)
    col_spec = P(None, ('rep', 'ep'), None, 'tp')
    down_spec = P(None, ('rep', 'ep'), 'tp', None)
    map_spec = P(None, None)

    def device_step(x_in, route_ids, gate_vals, w_gate, w_up, w_down, old_map, move_src, move_dst):
        layers, slots, width, part = w_gate.shape
        tokens, top_k = route_ids.shape[1], route_ids.shape[2]
        all_slots = group * slots
        cap = 2 * tokens * top_k // all_slots
        half = cap // 2
        feats = width // cols
        ep = lax.axis_index('ep')
        tp = lax.axis_index('tp')
        packed = jnp.stack([jnp.swapaxes(w_gate, 2, 3), jnp.swapaxes(w_up, 2, 3), w_down], axis=2)

        full = []
        for layer in range(layers):
            send = jnp.repeat(packed[layer], 2, axis=0)
            got = lax.all_to_all(send, 'tp', 0, 0, tiled=True)
            full.append([got[:, k].reshape(cols * part, width) for k in range(3)])

        tables = []
        expert_ids = jnp.arange(EXPERTS, dtype=jnp.int32)
        before = (jnp.arange(tokens)[:, None] < jnp.arange(tokens)[None, :]).astype(BF16)
        for layer in range(layers):
            ids = route_ids[layer].T
            match = ids[None, :, :] == expert_ids[:, None, None]
            taken = jnp.any(match, axis=1)
            gate = jnp.sum(jnp.where(match, gate_vals[layer].T[None], 0.0), axis=1)
            rank = jnp.dot(taken.astype(BF16), before, preferred_element_type=F32).astype(jnp.int32)
            rank = jnp.where(taken, rank, -1)
            slot_ids = jnp.arange(all_slots, dtype=jnp.int32)
            holds = old_map[layer][None, :] == expert_ids[:, None]
            first = jnp.min(jnp.where(holds, slot_ids[None, :], all_slots - 1), axis=1)
            my_slots = jnp.arange(group, dtype=jnp.int32) * slots + tp // 2
            serves = first[:, None] == my_slots[None, :]
            picked = jnp.sum(jnp.where(serves[:, :, None], rank[:, None, :] + 1, 0), axis=0) - 1
            row = jnp.arange(half, dtype=jnp.int32) + half * (tp % 2)
            pick = (picked[:, None, :] == row[None, :, None]).astype(BF16)
            tables.append((rank, gate, first, pick.reshape(group * half, tokens)))

        hidden = x_in
        hidden_dim = 0
        residual = lax.dynamic_slice_in_dim(x_in, tp * feats, feats, axis=1).T
        for layer in range(layers):
            rank, gate, first, pick = tables[layer]
            send = lax.dot_general(pick, hidden, (((1,), (hidden_dim,)), ((), ())), preferred_element_type=F32).astype(BF16)
            rows = lax.all_to_all(send.reshape(group, half, width), 'ep', 0, 0, tiled=True).reshape(group * half, width)
            wg, wu, wd = full[layer]
            gate_acc = lax.dot_general(rows, wg, (((1,), (1,)), ((), ())), preferred_element_type=F32)
            up_acc = lax.dot_general(rows, wu, (((1,), (1,)), ((), ())), preferred_element_type=F32)
            act = (jax.nn.silu(gate_acc) * up_acc).astype(BF16)
            out = jnp.dot(act, wd, preferred_element_type=F32).astype(BF16)
            back = lax.all_to_all(out.reshape(group, half, width), 'ep', 0, 0, tiled=True)
            back = back.reshape(group, half, cols, feats).transpose(2, 0, 1, 3)
            back = lax.all_to_all(back, 'tp', 0, 0, tiled=True)
            residual = combine(first, back, rank, gate, residual, cap, group, slots)
            hidden = lax.all_gather(residual, 'tp', axis=0, tiled=True)
            hidden_dim = 1
        y_out = hidden.T

        pieces = group // layers
        depth = 3 * part // pieces
        send = packed.reshape(layers, slots, pieces, depth, width).transpose(0, 2, 1, 3, 4).reshape(group, slots, depth, width)
        held = lax.all_to_all(send, 'ep', 0, 0, tiled=True).reshape(all_slots, depth, width)
        source = jnp.arange(all_slots, dtype=jnp.int32)
        my_layer = ep // pieces
        source = source.at[move_dst[my_layer]].set(move_src[my_layer])
        held = held[source].reshape(group, slots, depth, width)
        got = lax.all_to_all(held, 'ep', 0, 0, tiled=True)
        new = got.reshape(layers, pieces, slots, depth, width).transpose(0, 2, 1, 3, 4).reshape(layers, slots, 3, part, width)
        return y_out, jnp.swapaxes(new[:, :, 0], 2, 3), jnp.swapaxes(new[:, :, 1], 2, 3), new[:, :, 2]

    return jax.shard_map(device_step, mesh=mesh, in_specs=(row_spec, layer_spec, layer_spec, col_spec, col_spec, down_spec, map_spec, map_spec, map_spec), out_specs=(row_spec, col_spec, col_spec, down_spec), check_vma=False)
```

```python
import functools

import jax
import jax.numpy as jnp
from jax import lax
from jax.experimental import pallas as pl
from jax.experimental.pallas import tpu as pltpu
from jax.sharding import PartitionSpec as P

EXPERTS = 40
F32 = jnp.float32
BF16 = jnp.bfloat16
VMEM = pl.BlockSpec(memory_space=pltpu.VMEM)
SMEM = pl.BlockSpec(memory_space=pltpu.SMEM)
ANY = pl.BlockSpec(memory_space=pl.ANY)
MESH = pl.DeviceIdType.MESH


def exchange_kernel(group, cols, src_ref, dst_ref, send_sem, recv_sem):
    ep, tp = lax.axis_index('ep'), lax.axis_index('tp')
    me = ep * cols + tp
    total = group * cols

    def send(k, carry):
        to_ep = lax.rem(ep + lax.rem(k, group), group)
        to_tp = lax.rem(tp + k // group + lax.rem(k, group), cols)
        to = to_ep * cols + to_tp

        @pl.when(to != me)
        def _():
            pltpu.make_async_remote_copy(src_ref.at[to], dst_ref.at[me], send_sem, recv_sem, device_id={'tp': to_tp, 'ep': to_ep}, device_id_type=MESH).start()

        return carry

    lax.fori_loop(0, total, send, 0)
    pltpu.make_async_copy(src_ref.at[me], dst_ref.at[me], recv_sem).start()
    pltpu.make_async_copy(src_ref, dst_ref, recv_sem).wait()
    some = pl.ds(0, total - 1)
    pltpu.make_async_copy(src_ref.at[some], dst_ref.at[some], send_sem).wait()


def exchange(blocks, group, cols):
    return pl.pallas_call(
        functools.partial(exchange_kernel, group, cols),
        out_shape=jax.ShapeDtypeStruct(blocks.shape, blocks.dtype),
        in_specs=[ANY],
        out_specs=ANY,
        scratch_shapes=[pltpu.SemaphoreType.DMA, pltpu.SemaphoreType.DMA],
        compiler_params=pltpu.CompilerParams(has_side_effects=True),
        cost_estimate=pl.CostEstimate(flops=0, bytes_accessed=120 << 20, transcendentals=0),
    )(blocks)


def gather_kernel(cols, src_ref, dst_ref, send_sem, recv_sem):
    tp = lax.axis_index('tp')

    def send(k, carry):
        to = lax.rem(tp + k, cols)
        pltpu.make_async_remote_copy(src_ref, dst_ref.at[tp], send_sem, recv_sem, device_id={'tp': to}, device_id_type=MESH).start()
        return carry

    lax.fori_loop(1, cols, send, 0)
    pltpu.make_async_copy(src_ref, dst_ref.at[tp], recv_sem).start()
    pltpu.make_async_copy(dst_ref, dst_ref, recv_sem).wait()
    some = dst_ref.at[pl.ds(0, cols - 1)]
    pltpu.make_async_copy(some, some, send_sem).wait()


def gather_cols(block, cols):
    return pl.pallas_call(
        functools.partial(gather_kernel, cols),
        out_shape=jax.ShapeDtypeStruct((cols,) + block.shape, block.dtype),
        in_specs=[ANY],
        out_specs=ANY,
        scratch_shapes=[pltpu.SemaphoreType.DMA, pltpu.SemaphoreType.DMA],
        compiler_params=pltpu.CompilerParams(has_side_effects=True),
        cost_estimate=pl.CostEstimate(flops=0, bytes_accessed=120 << 20, transcendentals=0),
    )(block)


def expert_kernel(wide, rows_ref, mine_ref, other_ref, out_ref, down_ref):
    blocks = out_ref.shape[0]
    width = out_ref.shape[1]
    half = mine_ref.shape[0] * mine_ref.shape[2]

    def whole(k):
        return jnp.concatenate([mine_ref[:, k].reshape(half, width), other_ref[:, k].reshape(half, width)], axis=0)

    down_ref[...] = whole(2).T

    def step(i, carry):
        if wide:
            rows = jnp.concatenate([rows_ref[2 * i], rows_ref[2 * i + 1]], axis=1)
            dims = (((1,), (0,)), ((), ()))
        else:
            rows = jnp.concatenate([rows_ref[2 * i], rows_ref[2 * i + 1]], axis=0)
            dims = (((1,), (1,)), ((), ()))
        gate = lax.dot_general(whole(0), rows, dims, preferred_element_type=F32)
        up = lax.dot_general(whole(1), rows, dims, preferred_element_type=F32)
        act = (jax.nn.silu(gate) * up).astype(BF16)
        out = jnp.dot(down_ref[...], act, preferred_element_type=F32).astype(BF16)
        n = out_ref.shape[2]
        out_ref[2 * i] = out[:, :n]
        out_ref[2 * i + 1] = out[:, n:]
        return carry

    lax.fori_loop(0, blocks // 2, step, 0)


def run_expert(rows, mine, other, wide, width, half):
    blocks = rows.shape[0]
    ffn = 2 * mine.shape[0] * mine.shape[2]
    return pl.pallas_call(
        functools.partial(expert_kernel, wide),
        out_shape=jax.ShapeDtypeStruct((blocks, width, half), BF16),
        in_specs=[VMEM] * 3,
        out_specs=VMEM,
        scratch_shapes=[pltpu.VMEM((width, ffn), BF16)],
        cost_estimate=pl.CostEstimate(flops=6 * blocks * half * width * ffn, bytes_accessed=12 << 20, transcendentals=0),
    )(rows, mine, other)


def combine_kernel(cap, slots, cols, last, first_ref, next_ref, back_ref, rank_ref, gate_ref, nrank_ref, res_ref, out_ref, send_ref, acc_ref):
    tokens = rank_ref.shape[1]
    half = cap // 2
    acc_ref[...] = res_ref[...].astype(F32)
    row_iota = lax.broadcasted_iota(jnp.int32, (cap, tokens), 0)

    def step(expert, carry):
        slot = first_ref[expert]
        plane = slot // cols
        block = 2 * plane * cols + slot - plane * cols
        rows = jnp.concatenate([back_ref[block], back_ref[block + cols]], axis=1)
        pick = (rank_ref[pl.ds(expert, 1), :] == row_iota).astype(BF16)
        chosen = jnp.dot(rows, pick, preferred_element_type=F32)
        acc_ref[...] += gate_ref[pl.ds(expert, 1), :] * chosen
        return carry

    lax.fori_loop(0, EXPERTS, step, 0)
    out_ref[...] = acc_ref[...].astype(BF16)
    if last:
        return
    hidden = out_ref[...]

    def step2(expert, carry):
        slot = next_ref[expert]
        plane = slot // cols
        block = 2 * plane * cols + slot - plane * cols
        pick = (nrank_ref[pl.ds(expert, 1), :] == row_iota).astype(BF16)
        rows = lax.dot_general(hidden, pick, (((1,), (1,)), ((), ())), preferred_element_type=F32).astype(BF16)
        send_ref[block] = rows[:, :half]
        send_ref[block + cols] = rows[:, half:]
        return carry

    lax.fori_loop(0, EXPERTS, step2, 0)


def combine(first, nfirst, back, rank, gate, nrank, residual, cap, slots, cols, last):
    feats, tokens = residual.shape
    return pl.pallas_call(
        functools.partial(combine_kernel, cap, slots, cols, last),
        out_shape=(jax.ShapeDtypeStruct((feats, tokens), BF16), jax.ShapeDtypeStruct((8, 128) if last else back.shape, BF16)),
        in_specs=[SMEM] * 2 + [VMEM] * 5,
        out_specs=(VMEM, VMEM),
        scratch_shapes=[pltpu.VMEM((feats, tokens), F32)],
        cost_estimate=pl.CostEstimate(flops=2 * EXPERTS * cap * 256 * tokens, bytes_accessed=8 << 20, transcendentals=0),
    )(first, nfirst, back, rank, gate, nrank, residual)


def solution(mesh):
    group = mesh.shape['ep']
    cols = mesh.shape['tp']
    row_spec = P(('rep', 'ep'), None)
    layer_spec = P(None, ('rep', 'ep'), None)
    col_spec = P(None, ('rep', 'ep'), None, 'tp')
    down_spec = P(None, ('rep', 'ep'), 'tp', None)
    map_spec = P(None, None)

    def device_step(x_in, route_ids, gate_vals, w_gate, w_up, w_down, old_map, move_src, move_dst):
        layers, slots, width, part = w_gate.shape
        tokens, top_k = route_ids.shape[1], route_ids.shape[2]
        all_slots = group * slots
        cap = 2 * tokens * top_k // all_slots
        half = cap // 2
        feats = width // cols
        ep = lax.axis_index('ep')
        tp = lax.axis_index('tp')
        core = ep % 2
        partner = [(i, i ^ 1) for i in range(group)]
        packed = jnp.stack([jnp.swapaxes(w_gate, 2, 3), jnp.swapaxes(w_up, 2, 3), w_down], axis=2)

        full = []
        for layer in range(layers):
            cut = packed[layer].reshape(slots, 3, 2, part // 2, width)
            keep = lax.dynamic_index_in_dim(cut, core, 2, keepdims=False)
            give = lax.dynamic_index_in_dim(cut, 1 - core, 2, keepdims=False)
            take = lax.ppermute(give, 'ep', partner)
            send = jnp.where(core == 0, jnp.stack([keep, take]), jnp.stack([take, keep])).reshape(2 * slots, 3, part // 2, width)
            mine = lax.all_to_all(send, 'tp', 0, 0, tiled=True)
            full.append((mine, lax.ppermute(mine, 'ep', partner)))

        tables = []
        expert_ids = jnp.arange(EXPERTS, dtype=jnp.int32)
        before = (jnp.arange(tokens)[:, None] < jnp.arange(tokens)[None, :]).astype(BF16)
        for layer in range(layers):
            ids = route_ids[layer].T
            match = ids[None, :, :] == expert_ids[:, None, None]
            taken = jnp.any(match, axis=1)
            gate = jnp.sum(jnp.where(match, gate_vals[layer].T[None], 0.0), axis=1)
            rank = jnp.dot(taken.astype(BF16), before, preferred_element_type=F32).astype(jnp.int32)
            rank = jnp.where(taken, rank, -1)
            slot_ids = jnp.arange(all_slots, dtype=jnp.int32)
            holds = old_map[layer][None, :] == expert_ids[:, None]
            first = jnp.min(jnp.where(holds, slot_ids[None, :], all_slots - 1), axis=1)
            tables.append((rank, gate, first))

        rank, gate, first = tables[0]
        my_slots = jnp.arange(group // 2, dtype=jnp.int32) * cols + tp
        serves = first[:, None] == my_slots[None, :]
        picked = jnp.sum(jnp.where(serves[:, :, None], rank[:, None, :] + 1, 0), axis=0) - 1
        row = jnp.arange(cap, dtype=jnp.int32)
        pick = (picked[:, None, :] == row[None, :, None]).astype(BF16).reshape(group * half, tokens)
        send = jnp.dot(pick, x_in, preferred_element_type=F32).astype(BF16)
        rows = lax.all_to_all(send.reshape(group, half, width), 'ep', 0, 0, tiled=True)

        residual = lax.dynamic_slice_in_dim(x_in, tp * feats, feats, axis=1).T
        for layer in range(layers):
            last = layer == layers - 1
            rank, gate, first = tables[layer]
            nrank, _, nfirst = tables[layer if last else layer + 1]
            out = run_expert(rows, full[layer][0], full[layer][1], layer > 0, width, half)
            out = out.reshape(group, cols, feats, half).reshape(group * cols, feats, half)
            back = exchange(out, group, cols)
            residual, send = combine(first, nfirst, back, rank, gate, nrank, residual, cap, slots, cols, last)
            if not last:
                rows = exchange(send, group, cols).reshape(group, width, half)
        y_out = gather_cols(residual, cols).reshape(width, tokens).T

        pieces = group // layers
        depth = 3 * part // pieces
        send = packed.reshape(layers, slots, pieces, depth, width).transpose(0, 2, 1, 3, 4).reshape(group, slots, depth, width)
        held = lax.all_to_all(send, 'ep', 0, 0, tiled=True).reshape(all_slots, depth, width)
        source = jnp.arange(all_slots, dtype=jnp.int32)
        my_layer = ep // pieces
        source = source.at[move_dst[my_layer]].set(move_src[my_layer])
        held = held[source].reshape(group, slots, depth, width)
        got = lax.all_to_all(held, 'ep', 0, 0, tiled=True)
        new = got.reshape(layers, pieces, slots, depth, width).transpose(0, 2, 1, 3, 4).reshape(layers, slots, 3, part, width)
        return y_out, jnp.swapaxes(new[:, :, 0], 2, 3), jnp.swapaxes(new[:, :, 1], 2, 3), new[:, :, 2]

    return jax.shard_map(device_step, mesh=mesh, in_specs=(row_spec, layer_spec, layer_spec, col_spec, col_spec, down_spec, map_spec, map_spec, map_spec), out_specs=(row_spec, col_spec, col_spec, down_spec), check_vma=False)
```

```python
import functools

import jax
import jax.numpy as jnp
from jax import lax
from jax.experimental import pallas as pl
from jax.experimental.pallas import tpu as pltpu
from jax.sharding import PartitionSpec as P

EXPERTS = 40
F32 = jnp.float32
BF16 = jnp.bfloat16
VMEM = pl.BlockSpec(memory_space=pltpu.VMEM)
SMEM = pl.BlockSpec(memory_space=pltpu.SMEM)
ANY = pl.BlockSpec(memory_space=pl.ANY)
MESH = pl.DeviceIdType.MESH
DMA = pltpu.SemaphoreType.DMA


def params(collective):
    return pltpu.CompilerParams(has_side_effects=True, collective_id=collective)


def signal_all(group, cols):
    ep, tp = lax.axis_index('ep'), lax.axis_index('tp')
    barrier = pltpu.get_barrier_semaphore()

    def tell(k, carry):
        peer = {'tp': lax.rem(tp + k // group, cols), 'ep': lax.rem(ep + lax.rem(k, group), group)}
        pl.semaphore_signal(barrier, inc=1, device_id=peer, device_id_type=MESH)
        return carry

    lax.fori_loop(1, group * cols, tell, 0)


def wait_all(group, cols):
    pl.semaphore_wait(pltpu.get_barrier_semaphore(), group * cols - 1)


def post(src, dst, to_ep, to_tp, send_sem, recv_sem):
    ep, tp = lax.axis_index('ep'), lax.axis_index('tp')
    here = jnp.logical_and(to_ep == ep, to_tp == tp)

    @pl.when(jnp.logical_not(here))
    def _():
        pltpu.make_async_remote_copy(src, dst, send_sem, recv_sem, device_id={'tp': to_tp, 'ep': to_ep}, device_id_type=MESH).start()

    @pl.when(here)
    def _():
        pltpu.make_async_copy(src, dst, recv_sem).start()


def await_bytes(ref, sem):
    pltpu.make_async_copy(ref, ref, sem).wait()


def front_kernel(group, cols, send_ref, w_ref, rows_ref, mine_ref, other_ref, rsend, rrecv, wsend, wrecv, osend, orecv):
    ep, tp = lax.axis_index('ep'), lax.axis_index('tp')
    core = lax.rem(ep, 2)
    slots = w_ref.shape[0]
    signal_all(group, cols)
    wait_all(group, cols)

    def weights(k, carry):
        slot = lax.rem(tp + k // 2, slots)
        half = lax.rem(k, 2)
        post(w_ref.at[slot, :, half], mine_ref.at[tp], ep - core + half, slots * core + slot, wsend, wrecv)
        return carry

    lax.fori_loop(0, 2 * slots, weights, 0)

    def rows(k, carry):
        to = lax.rem(ep + k, group)
        post(send_ref.at[to], rows_ref.at[ep], to, tp, rsend, rrecv)
        return carry

    lax.fori_loop(0, group, rows, 0)
    await_bytes(mine_ref, wrecv)
    swap = pltpu.make_async_remote_copy(mine_ref, other_ref, osend, orecv, device_id={'ep': ep + 1 - 2 * core}, device_id_type=MESH)
    swap.start()
    await_bytes(rows_ref, rrecv)
    await_bytes(rows_ref.at[pl.ds(0, group - 1)], rsend)
    own = tp // slots == core

    @pl.when(own)
    def _():
        await_bytes(mine_ref.at[pl.ds(0, 2 * slots - 1)], wsend)

    @pl.when(jnp.logical_not(own))
    def _():
        await_bytes(mine_ref, wsend)

    swap.wait()


def run_front(send, weights, group, cols, collective):
    slots, mats, _, part, width = weights.shape
    piece = jax.ShapeDtypeStruct((cols, mats, part, width), BF16)
    return pl.pallas_call(
        functools.partial(front_kernel, group, cols),
        out_shape=(jax.ShapeDtypeStruct(send.shape, BF16), piece, piece),
        in_specs=[ANY] * 2,
        out_specs=(ANY,) * 3,
        scratch_shapes=[DMA] * 6,
        compiler_params=params(collective),
        cost_estimate=pl.CostEstimate(flops=0, bytes_accessed=120 << 20, transcendentals=0),
    )(send, weights)


def expert_kernel(group, cols, wide, rows_ref, mine_ref, other_ref, dst_ref, out_ref, down_ref, send_sem, recv_sem):
    ep, tp = lax.axis_index('ep'), lax.axis_index('tp')
    me = ep * cols + tp
    width = mine_ref.shape[3]
    half = mine_ref.shape[0] * mine_ref.shape[2]
    feats, n = out_ref.shape[1:]
    pairs = group // 2
    signal_all(group, cols)

    def whole(k):
        return jnp.concatenate([mine_ref[:, k].reshape(half, width), other_ref[:, k].reshape(half, width)], axis=0)

    def plane(i):
        return lax.rem(ep // 2 + 1 + i, pairs)

    def compute(i):
        at = 2 * plane(i)
        rows = jnp.concatenate([rows_ref[at], rows_ref[at + 1]], axis=1 if wide else 0)
        dims = (((1,), (0 if wide else 1,)), ((), ()))
        gate = lax.dot_general(whole(0), rows, dims, preferred_element_type=F32)
        up = lax.dot_general(whole(1), rows, dims, preferred_element_type=F32)
        act = (jax.nn.silu(gate) * up).astype(BF16)
        out = jnp.dot(down_ref[...], act, preferred_element_type=F32).astype(BF16)
        out_ref[pl.ds(at * cols, cols)] = out[:, :n].reshape(cols, feats, n)
        out_ref[pl.ds((at + 1) * cols, cols)] = out[:, n:].reshape(cols, feats, n)

    def send(i):
        at = 2 * plane(i)

        def one(k, carry):
            to_ep = at + lax.rem(k, 2)
            to_tp = lax.rem(tp + k // 2, cols)
            post(out_ref.at[to_ep * cols + to_tp], dst_ref.at[me], to_ep, to_tp, send_sem, recv_sem)
            return carry

        lax.fori_loop(0, 2 * cols, one, 0)

    down_ref[...] = whole(2).T
    compute(0)
    wait_all(group, cols)

    def step(i, carry):
        compute(i)
        send(i - 1)
        return carry

    lax.fori_loop(1, pairs, step, 0)
    send(pairs - 1)
    await_bytes(dst_ref, recv_sem)
    await_bytes(dst_ref.at[pl.ds(0, group * cols - 1)], send_sem)


def run_expert(rows, mine, other, wide, width, half, group, cols, collective):
    ffn = 2 * mine.shape[0] * mine.shape[2]
    blocks = (group * cols, width // cols, half)
    return pl.pallas_call(
        functools.partial(expert_kernel, group, cols, wide),
        out_shape=jax.ShapeDtypeStruct(blocks, BF16),
        in_specs=[VMEM] * 3,
        out_specs=ANY,
        scratch_shapes=[pltpu.VMEM(blocks, BF16), pltpu.VMEM((width, ffn), BF16), DMA, DMA],
        compiler_params=params(collective),
        cost_estimate=pl.CostEstimate(flops=6 * group * half * width * ffn, bytes_accessed=120 << 20, transcendentals=0),
    )(rows, mine, other)


def weigh(cap, cols, first_ref, back_ref, rank_ref, gate_ref, res_ref, acc_ref):
    tokens = rank_ref.shape[1]
    acc_ref[...] = res_ref[...].astype(F32)
    row_iota = lax.broadcasted_iota(jnp.int32, (cap, tokens), 0)

    def step(expert, carry):
        slot = first_ref[expert]
        plane = slot // cols
        block = plane * cols + slot
        rows = jnp.concatenate([back_ref[block], back_ref[block + cols]], axis=1)
        pick = (rank_ref[pl.ds(expert, 1), :] == row_iota).astype(BF16)
        chosen = jnp.dot(rows, pick, preferred_element_type=F32)
        acc_ref[...] += gate_ref[pl.ds(expert, 1), :] * chosen
        return carry

    lax.fori_loop(0, EXPERTS, step, 0)


def middle_kernel(group, cols, cap, first_ref, back_ref, rank_ref, gate_ref, nrank_ref, res_ref, out_ref, dst_ref, send_ref, acc_ref, send_sem, recv_sem):
    ep, tp = lax.axis_index('ep'), lax.axis_index('tp')
    me = ep * cols + tp
    tokens = rank_ref.shape[1]
    half = cap // 2
    all_slots = nrank_ref.shape[0]
    signal_all(group, cols)
    weigh(cap, cols, first_ref, back_ref, rank_ref, gate_ref, res_ref, acc_ref)
    out_ref[...] = acc_ref[...].astype(BF16)
    wait_all(group, cols)
    row_iota = lax.broadcasted_iota(jnp.int32, (cap, tokens), 0)

    def place(i):
        plane = lax.rem(ep // 2 + 1 + lax.rem(i, group // 2), group // 2)
        column = lax.rem(tp + i // (group // 2), cols)
        return plane, column

    def compute(i):
        plane, column = place(i)
        pick = (nrank_ref[pl.ds(plane * cols + column, 1), :] == row_iota).astype(BF16)
        rows = lax.dot_general(out_ref[...], pick, (((1,), (1,)), ((), ())), preferred_element_type=F32).astype(BF16)
        block = 2 * plane * cols + column
        send_ref[block] = rows[:, :half]
        send_ref[block + cols] = rows[:, half:]

    def send(i):
        plane, column = place(i)
        block = 2 * plane * cols + column
        post(send_ref.at[block], dst_ref.at[me], 2 * plane, column, send_sem, recv_sem)
        post(send_ref.at[block + cols], dst_ref.at[me], 2 * plane + 1, column, send_sem, recv_sem)

    compute(0)

    def step(i, carry):
        compute(i)
        send(i - 1)
        return carry

    lax.fori_loop(1, all_slots, step, 0)
    send(all_slots - 1)
    await_bytes(dst_ref, recv_sem)
    await_bytes(dst_ref.at[pl.ds(0, group * cols - 1)], send_sem)


def run_middle(first, back, rank, gate, nrank, residual, group, cols, cap, collective):
    feats, tokens = residual.shape
    return pl.pallas_call(
        functools.partial(middle_kernel, group, cols, cap),
        out_shape=(jax.ShapeDtypeStruct((feats, tokens), BF16), jax.ShapeDtypeStruct(back.shape, BF16)),
        in_specs=[SMEM] + [VMEM] * 5,
        out_specs=(VMEM, ANY),
        scratch_shapes=[pltpu.VMEM(back.shape, BF16), pltpu.VMEM((feats, tokens), F32), DMA, DMA],
        compiler_params=params(collective),
        cost_estimate=pl.CostEstimate(flops=2 * EXPERTS * cap * 256 * tokens, bytes_accessed=120 << 20, transcendentals=0),
    )(first, back, rank, gate, nrank, residual)


def last_kernel(group, cols, side, cap, first_ref, back_ref, rank_ref, gate_ref, res_ref, dst_ref, out_ref, acc_ref, own_sem, send_sem, recv_sem):
    ep, tp = lax.axis_index('ep'), lax.axis_index('tp')
    z, y = tp // side, lax.rem(tp, side)
    feats = out_ref.shape[0]
    cut = feats // 2
    low, high = pl.ds(0, cut), pl.ds(cut, cut)
    signal_all(group, cols)
    weigh(cap, cols, first_ref, back_ref, rank_ref, gate_ref, res_ref, acc_ref)
    out_ref[...] = acc_ref[...].astype(BF16)
    own = pltpu.make_async_copy(out_ref, dst_ref.at[z, y], own_sem)
    own.start()
    own.wait()
    wait_all(group, cols)

    def push(ref, to_z, to_y, k):
        pltpu.make_async_remote_copy(ref, ref, send_sem.at[k], recv_sem.at[k], device_id={'tp': to_z * side + to_y}, device_id_type=MESH).start()

    for j in range(1, side):
        push(dst_ref.at[z, y, low], z, lax.rem(y + j, side), 0)
        push(dst_ref.at[z, y, high], lax.rem(z + j, side), y, 1)
    some = pl.ds(0, side - 1)
    await_bytes(dst_ref.at[z, some, low], recv_sem.at[0])
    for j in range(1, side):
        push(dst_ref.at[z, :, low], lax.rem(z + j, side), y, 2)
    await_bytes(dst_ref.at[some, y, high], recv_sem.at[1])
    for j in range(1, side):
        push(dst_ref.at[:, y, high], z, lax.rem(y + j, side), 3)
    await_bytes(dst_ref.at[some, :, low], recv_sem.at[2])
    await_bytes(dst_ref.at[:, some, high], recv_sem.at[3])
    await_bytes(dst_ref.at[z, some, low], send_sem.at[0])
    await_bytes(dst_ref.at[some, y, high], send_sem.at[1])
    await_bytes(dst_ref.at[some, :, low], send_sem.at[2])
    await_bytes(dst_ref.at[:, some, high], send_sem.at[3])


def run_last(first, back, rank, gate, residual, group, cols, cap, collective):
    feats, tokens = residual.shape
    side = int(round(cols ** 0.5))
    return pl.pallas_call(
        functools.partial(last_kernel, group, cols, side, cap),
        out_shape=jax.ShapeDtypeStruct((side, side, feats, tokens), BF16),
        in_specs=[SMEM] + [VMEM] * 4,
        out_specs=ANY,
        scratch_shapes=[pltpu.VMEM((feats, tokens), BF16), pltpu.VMEM((feats, tokens), F32), DMA, DMA((4,)), DMA((4,))],
        compiler_params=params(collective),
        cost_estimate=pl.CostEstimate(flops=2 * EXPERTS * cap * 256 * tokens, bytes_accessed=120 << 20, transcendentals=0),
    )(first, back, rank, gate, residual)


def solution(mesh):
    group = mesh.shape['ep']
    cols = mesh.shape['tp']
    row_spec = P(('rep', 'ep'), None)
    layer_spec = P(None, ('rep', 'ep'), None)
    col_spec = P(None, ('rep', 'ep'), None, 'tp')
    down_spec = P(None, ('rep', 'ep'), 'tp', None)
    map_spec = P(None, None)

    def device_step(x_in, route_ids, gate_vals, w_gate, w_up, w_down, old_map, move_src, move_dst):
        layers, slots, width, part = w_gate.shape
        tokens, top_k = route_ids.shape[1], route_ids.shape[2]
        all_slots = group * slots
        cap = 2 * tokens * top_k // all_slots
        half = cap // 2
        feats = width // cols
        ep = lax.axis_index('ep')
        tp = lax.axis_index('tp')
        core = ep % 2
        partner = [(i, i ^ 1) for i in range(group)]
        packed = jnp.stack([jnp.swapaxes(w_gate, 2, 3), jnp.swapaxes(w_up, 2, 3), w_down], axis=2)

        tables = []
        expert_ids = jnp.arange(EXPERTS, dtype=jnp.int32)
        slot_ids = jnp.arange(all_slots, dtype=jnp.int32)
        before = (jnp.arange(tokens)[:, None] < jnp.arange(tokens)[None, :]).astype(BF16)
        for layer in range(layers):
            ids = route_ids[layer].T
            match = ids[None, :, :] == expert_ids[:, None, None]
            taken = jnp.any(match, axis=1)
            gate = jnp.sum(jnp.where(match, gate_vals[layer].T[None], 0.0), axis=1)
            rank = jnp.dot(taken.astype(BF16), before, preferred_element_type=F32).astype(jnp.int32)
            rank = jnp.where(taken, rank, -1)
            holds = old_map[layer][None, :] == expert_ids[:, None]
            first = jnp.min(jnp.where(holds, slot_ids[None, :], all_slots - 1), axis=1)
            tables.append((rank, gate, first))

        rank, gate, first = tables[0]
        my_slots = jnp.arange(group // 2, dtype=jnp.int32) * cols + tp
        serves = first[:, None] == my_slots[None, :]
        picked = jnp.sum(jnp.where(serves[:, :, None], rank[:, None, :] + 1, 0), axis=0) - 1
        row = jnp.arange(cap, dtype=jnp.int32)
        pick = (picked[:, None, :] == row[None, :, None]).astype(BF16).reshape(group * half, tokens)
        send = jnp.dot(pick, x_in, preferred_element_type=F32).astype(BF16).reshape(group, half, width)
        cut = packed.reshape(layers, slots, 3, 2, part // 2, width)
        rows, mine, other = run_front(send, cut[0], group, cols, 0)
        rows, later = lax.optimization_barrier((rows, packed))

        cut1 = later.reshape(layers, slots, 3, 2, part // 2, width)[1]
        keep = lax.dynamic_index_in_dim(cut1, core, 2, keepdims=False)
        give = lax.dynamic_index_in_dim(cut1, 1 - core, 2, keepdims=False)
        take = lax.ppermute(give, 'ep', partner)
        wsend = jnp.where(core == 0, jnp.stack([keep, take]), jnp.stack([take, keep])).reshape(2 * slots, 3, part // 2, width)
        mine1 = lax.all_to_all(wsend, 'tp', 0, 0, tiled=True)
        residual = lax.dynamic_slice_in_dim(x_in, tp * feats, feats, axis=1).T
        nrank, ngate, nfirst = tables[1]
        serving = (nfirst[:, None] == slot_ids[None, :])
        by_slot = jnp.sum(jnp.where(serving[:, :, None], nrank[:, None, :] + 1, 0), axis=0) - 1
        back = run_expert(rows, mine, other, False, width, half, group, cols, 1)
        back, mine1, later = lax.optimization_barrier((back, mine1, later))
        other1 = lax.ppermute(mine1, 'ep', partner)

        pieces = group // layers
        depth = 3 * part // pieces
        cut2 = later.reshape(layers, slots, pieces, depth, width).transpose(0, 2, 1, 3, 4).reshape(group, slots, depth, width)
        held = lax.all_to_all(cut2, 'ep', 0, 0, tiled=True).reshape(all_slots, depth, width)

        residual, rows = run_middle(first, back, rank, gate, by_slot, residual, group, cols, cap, 2)
        rows, other1, held = lax.optimization_barrier((rows, other1, held))
        source = jnp.arange(all_slots, dtype=jnp.int32)
        my_layer = ep // pieces
        source = source.at[move_dst[my_layer]].set(move_src[my_layer])
        got = lax.all_to_all(held[source].reshape(group, slots, depth, width), 'ep', 0, 0, tiled=True)

        rows = rows.reshape(group, width, half)
        back = run_expert(rows, mine1, other1, True, width, half, group, cols, 3)
        y_out = run_last(nfirst, back, nrank, ngate, residual, group, cols, cap, 4).reshape(width, tokens).T

        new = got.reshape(layers, pieces, slots, depth, width).transpose(0, 2, 1, 3, 4).reshape(layers, slots, 3, part, width)
        return y_out, jnp.swapaxes(new[:, :, 0], 2, 3), jnp.swapaxes(new[:, :, 1], 2, 3), new[:, :, 2]

    return jax.shard_map(device_step, mesh=mesh, in_specs=(row_spec, layer_spec, layer_spec, col_spec, col_spec, down_spec, map_spec, map_spec, map_spec), out_specs=(row_spec, col_spec, col_spec, down_spec), check_vma=False)
```

```python
import functools

import jax
import jax.numpy as jnp
from jax import lax
from jax.experimental import pallas as pl
from jax.experimental.pallas import tpu as pltpu
from jax.sharding import PartitionSpec as P

EXPERTS = 40
F32 = jnp.float32
BF16 = jnp.bfloat16
VMEM = pl.BlockSpec(memory_space=pltpu.VMEM)
SMEM = pl.BlockSpec(memory_space=pltpu.SMEM)
ANY = pl.BlockSpec(memory_space=pl.ANY)
MESH = pl.DeviceIdType.MESH
DMA = pltpu.SemaphoreType.DMA


def params(collective):
    return pltpu.CompilerParams(has_side_effects=True, collective_id=collective)


def signal_all(group, cols):
    ep, tp = lax.axis_index('ep'), lax.axis_index('tp')
    barrier = pltpu.get_barrier_semaphore()

    def tell(k, carry):
        peer = {'tp': lax.rem(tp + k // group, cols), 'ep': lax.rem(ep + lax.rem(k, group), group)}
        pl.semaphore_signal(barrier, inc=1, device_id=peer, device_id_type=MESH)
        return carry

    lax.fori_loop(1, group * cols, tell, 0)


def wait_all(group, cols):
    pl.semaphore_wait(pltpu.get_barrier_semaphore(), group * cols - 1)


def post(src, dst, to_ep, to_tp, send_sem, recv_sem):
    ep, tp = lax.axis_index('ep'), lax.axis_index('tp')
    here = jnp.logical_and(to_ep == ep, to_tp == tp)

    @pl.when(jnp.logical_not(here))
    def _():
        pltpu.make_async_remote_copy(src, dst, send_sem, recv_sem, device_id={'tp': to_tp, 'ep': to_ep}, device_id_type=MESH).start()

    @pl.when(here)
    def _():
        pltpu.make_async_copy(src, dst, recv_sem).start()


def await_bytes(ref, sem):
    pltpu.make_async_copy(ref, ref, sem).wait()


def front_kernel(group, cols, cap, x_ref, picked_ref, g_ref, u_ref, d_ref, rows_ref, mine0_ref, other0_ref, mine1_ref, other1_ref, send_ref, rsend, rrecv, wsend, wrecv, osend, orecv):
    ep, tp = lax.axis_index('ep'), lax.axis_index('tp')
    core = lax.rem(ep, 2)
    slots = g_ref.shape[1]
    half = cap // 2
    mines, others = (mine0_ref, mine1_ref), (other0_ref, other1_ref)
    signal_all(group, cols)
    row_iota = lax.broadcasted_iota(jnp.int32, (cap, x_ref.shape[0]), 0)

    def compute(i, carry):
        pick = (picked_ref[pl.ds(i, 1), :] == row_iota).astype(BF16)
        rows = jnp.dot(pick, x_ref[...], preferred_element_type=F32).astype(BF16)
        send_ref[2 * i] = rows[:half]
        send_ref[2 * i + 1] = rows[half:]
        return carry

    lax.fori_loop(0, group // 2, compute, 0)
    wait_all(group, cols)

    def weights(layer):
        def one(k, carry):
            slot = lax.rem(tp + k // 2, slots)
            part = lax.rem(k, 2)
            for mat, ref in enumerate((g_ref, u_ref, d_ref)):
                post(ref.at[layer, slot, part], mines[layer].at[tp, mat], ep - core + part, slots * core + slot, wsend.at[layer], wrecv.at[layer])
            return carry

        lax.fori_loop(0, 2 * slots, one, 0)

    def rows(k, carry):
        to = lax.rem(ep + k, group)
        post(send_ref.at[to], rows_ref.at[ep], to, tp, rsend, rrecv)
        return carry

    weights(0)
    lax.fori_loop(0, group, rows, 0)
    weights(1)
    swaps = []
    for layer in range(2):
        await_bytes(mines[layer], wrecv.at[layer])
        swap = pltpu.make_async_remote_copy(mines[layer], others[layer], osend.at[layer], orecv.at[layer], device_id={'ep': ep + 1 - 2 * core}, device_id_type=MESH)
        swap.start()
        swaps.append(swap)
    await_bytes(rows_ref, rrecv)
    await_bytes(rows_ref.at[pl.ds(0, group - 1)], rsend)
    own = tp // slots == core
    for layer in range(2):
        @pl.when(own)
        def _():
            await_bytes(mines[layer].at[pl.ds(0, 2 * slots - 1)], wsend.at[layer])

        @pl.when(jnp.logical_not(own))
        def _():
            await_bytes(mines[layer], wsend.at[layer])

        swaps[layer].wait()


def run_front(x, picked, gates, ups, downs, group, cols, cap, collective):
    _, slots, _, part, width = gates.shape
    piece = jax.ShapeDtypeStruct((cols, 3, part, width), BF16)
    rows = (group, cap // 2, width)
    return pl.pallas_call(
        functools.partial(front_kernel, group, cols, cap),
        out_shape=(jax.ShapeDtypeStruct(rows, BF16),) + (piece,) * 4,
        in_specs=[VMEM] * 2 + [ANY] * 3,
        out_specs=(ANY,) * 5,
        scratch_shapes=[pltpu.VMEM(rows, BF16), DMA, DMA] + [DMA((2,))] * 4,
        compiler_params=params(collective),
        cost_estimate=pl.CostEstimate(flops=0, bytes_accessed=240 << 20, transcendentals=0),
    )(x, picked, gates, ups, downs)


def expert_kernel(group, cols, wide, rows_ref, mine_ref, other_ref, dst_ref, out_ref, down_ref, send_sem, recv_sem):
    ep, tp = lax.axis_index('ep'), lax.axis_index('tp')
    me = ep * cols + tp
    width = mine_ref.shape[3]
    half = mine_ref.shape[0] * mine_ref.shape[2]
    feats, n = out_ref.shape[1:]
    pairs = group // 2
    signal_all(group, cols)

    def whole(k):
        return jnp.concatenate([mine_ref[:, k].reshape(half, width), other_ref[:, k].reshape(half, width)], axis=0)

    def plane(i):
        return lax.rem(ep // 2 + 1 + i, pairs)

    def compute(i):
        at = 2 * plane(i)
        rows = jnp.concatenate([rows_ref[at], rows_ref[at + 1]], axis=1 if wide else 0)
        dims = (((1,), (0 if wide else 1,)), ((), ()))
        gate = lax.dot_general(whole(0), rows, dims, preferred_element_type=F32)
        up = lax.dot_general(whole(1), rows, dims, preferred_element_type=F32)
        act = (jax.nn.silu(gate) * up).astype(BF16)
        out = jnp.dot(down_ref[...], act, preferred_element_type=F32).astype(BF16)
        out_ref[pl.ds(at * cols, cols)] = out[:, :n].reshape(cols, feats, n)
        out_ref[pl.ds((at + 1) * cols, cols)] = out[:, n:].reshape(cols, feats, n)

    def send(i):
        at = 2 * plane(i)

        def one(k, carry):
            to_ep = at + lax.rem(k, 2)
            to_tp = lax.rem(tp + k // 2, cols)
            post(out_ref.at[to_ep * cols + to_tp], dst_ref.at[me], to_ep, to_tp, send_sem, recv_sem)
            return carry

        lax.fori_loop(0, 2 * cols, one, 0)

    down_ref[...] = whole(2).T
    compute(0)
    wait_all(group, cols)

    def step(i, carry):
        compute(i)
        send(i - 1)
        return carry

    lax.fori_loop(1, pairs, step, 0)
    send(pairs - 1)
    await_bytes(dst_ref, recv_sem)
    await_bytes(dst_ref.at[pl.ds(0, group * cols - 1)], send_sem)


def run_expert(rows, mine, other, wide, width, half, group, cols, collective):
    ffn = 2 * mine.shape[0] * mine.shape[2]
    blocks = (group * cols, width // cols, half)
    return pl.pallas_call(
        functools.partial(expert_kernel, group, cols, wide),
        out_shape=jax.ShapeDtypeStruct(blocks, BF16),
        in_specs=[VMEM] * 3,
        out_specs=ANY,
        scratch_shapes=[pltpu.VMEM(blocks, BF16), pltpu.VMEM((width, ffn), BF16), DMA, DMA],
        compiler_params=params(collective),
        cost_estimate=pl.CostEstimate(flops=6 * group * half * width * ffn, bytes_accessed=120 << 20, transcendentals=0),
    )(rows, mine, other)


def weigh(cap, cols, first_ref, back_ref, rank_ref, gate_ref, res_ref, acc_ref):
    tokens = rank_ref.shape[1]
    acc_ref[...] = res_ref[...].astype(F32)
    row_iota = lax.broadcasted_iota(jnp.int32, (cap, tokens), 0)

    def step(expert, carry):
        slot = first_ref[expert]
        plane = slot // cols
        block = plane * cols + slot
        rows = jnp.concatenate([back_ref[block], back_ref[block + cols]], axis=1)
        pick = (rank_ref[pl.ds(expert, 1), :] == row_iota).astype(BF16)
        chosen = jnp.dot(rows, pick, preferred_element_type=F32)
        acc_ref[...] += gate_ref[pl.ds(expert, 1), :] * chosen
        return carry

    lax.fori_loop(0, EXPERTS, step, 0)


def middle_kernel(group, cols, cap, first_ref, back_ref, rank_ref, gate_ref, nrank_ref, res_ref, out_ref, dst_ref, send_ref, acc_ref, send_sem, recv_sem):
    ep, tp = lax.axis_index('ep'), lax.axis_index('tp')
    me = ep * cols + tp
    tokens = rank_ref.shape[1]
    half = cap // 2
    all_slots = nrank_ref.shape[0]
    signal_all(group, cols)
    weigh(cap, cols, first_ref, back_ref, rank_ref, gate_ref, res_ref, acc_ref)
    out_ref[...] = acc_ref[...].astype(BF16)
    wait_all(group, cols)
    row_iota = lax.broadcasted_iota(jnp.int32, (cap, tokens), 0)

    def place(i):
        plane = lax.rem(ep // 2 + 1 + lax.rem(i, group // 2), group // 2)
        column = lax.rem(tp + i // (group // 2), cols)
        return plane, column

    def compute(i):
        plane, column = place(i)
        pick = (nrank_ref[pl.ds(plane * cols + column, 1), :] == row_iota).astype(BF16)
        rows = lax.dot_general(out_ref[...], pick, (((1,), (1,)), ((), ())), preferred_element_type=F32).astype(BF16)
        block = 2 * plane * cols + column
        send_ref[block] = rows[:, :half]
        send_ref[block + cols] = rows[:, half:]

    def send(i):
        plane, column = place(i)
        block = 2 * plane * cols + column
        post(send_ref.at[block], dst_ref.at[me], 2 * plane, column, send_sem, recv_sem)
        post(send_ref.at[block + cols], dst_ref.at[me], 2 * plane + 1, column, send_sem, recv_sem)

    compute(0)

    def step(i, carry):
        compute(i)
        send(i - 1)
        return carry

    lax.fori_loop(1, all_slots, step, 0)
    send(all_slots - 1)
    await_bytes(dst_ref, recv_sem)
    await_bytes(dst_ref.at[pl.ds(0, group * cols - 1)], send_sem)


def run_middle(first, back, rank, gate, nrank, residual, group, cols, cap, collective):
    feats, tokens = residual.shape
    return pl.pallas_call(
        functools.partial(middle_kernel, group, cols, cap),
        out_shape=(jax.ShapeDtypeStruct((feats, tokens), BF16), jax.ShapeDtypeStruct(back.shape, BF16)),
        in_specs=[SMEM] + [VMEM] * 5,
        out_specs=(VMEM, ANY),
        scratch_shapes=[pltpu.VMEM(back.shape, BF16), pltpu.VMEM((feats, tokens), F32), DMA, DMA],
        compiler_params=params(collective),
        cost_estimate=pl.CostEstimate(flops=2 * EXPERTS * cap * 256 * tokens, bytes_accessed=120 << 20, transcendentals=0),
    )(first, back, rank, gate, nrank, residual)


def last_kernel(group, cols, side, cap, first_ref, back_ref, rank_ref, gate_ref, res_ref, dst_ref, out_ref, acc_ref, own_sem, send_sem, recv_sem):
    ep, tp = lax.axis_index('ep'), lax.axis_index('tp')
    z, y = tp // side, lax.rem(tp, side)
    feats = out_ref.shape[0]
    cut = feats // 2
    low, high = pl.ds(0, cut), pl.ds(cut, cut)
    signal_all(group, cols)
    weigh(cap, cols, first_ref, back_ref, rank_ref, gate_ref, res_ref, acc_ref)
    out_ref[...] = acc_ref[...].astype(BF16)
    own = pltpu.make_async_copy(out_ref, dst_ref.at[z, y], own_sem)
    own.start()
    own.wait()
    wait_all(group, cols)

    def push(ref, to_z, to_y, k):
        pltpu.make_async_remote_copy(ref, ref, send_sem.at[k], recv_sem.at[k], device_id={'tp': to_z * side + to_y}, device_id_type=MESH).start()

    for j in range(1, side):
        push(dst_ref.at[z, y, low], z, lax.rem(y + j, side), 0)
        push(dst_ref.at[z, y, high], lax.rem(z + j, side), y, 1)
    some = pl.ds(0, side - 1)
    await_bytes(dst_ref.at[z, some, low], recv_sem.at[0])
    for j in range(1, side):
        push(dst_ref.at[z, :, low], lax.rem(z + j, side), y, 2)
    await_bytes(dst_ref.at[some, y, high], recv_sem.at[1])
    for j in range(1, side):
        push(dst_ref.at[:, y, high], z, lax.rem(y + j, side), 3)
    await_bytes(dst_ref.at[some, :, low], recv_sem.at[2])
    await_bytes(dst_ref.at[:, some, high], recv_sem.at[3])
    await_bytes(dst_ref.at[z, some, low], send_sem.at[0])
    await_bytes(dst_ref.at[some, y, high], send_sem.at[1])
    await_bytes(dst_ref.at[some, :, low], send_sem.at[2])
    await_bytes(dst_ref.at[:, some, high], send_sem.at[3])


def run_last(first, back, rank, gate, residual, group, cols, cap, collective):
    feats, tokens = residual.shape
    side = int(round(cols ** 0.5))
    return pl.pallas_call(
        functools.partial(last_kernel, group, cols, side, cap),
        out_shape=jax.ShapeDtypeStruct((side, side, feats, tokens), BF16),
        in_specs=[SMEM] + [VMEM] * 4,
        out_specs=ANY,
        scratch_shapes=[pltpu.VMEM((feats, tokens), BF16), pltpu.VMEM((feats, tokens), F32), DMA, DMA((4,)), DMA((4,))],
        compiler_params=params(collective),
        cost_estimate=pl.CostEstimate(flops=2 * EXPERTS * cap * 256 * tokens, bytes_accessed=120 << 20, transcendentals=0),
    )(first, back, rank, gate, residual)


def solution(mesh):
    group = mesh.shape['ep']
    cols = mesh.shape['tp']
    row_spec = P(('rep', 'ep'), None)
    layer_spec = P(None, ('rep', 'ep'), None)
    col_spec = P(None, ('rep', 'ep'), None, 'tp')
    down_spec = P(None, ('rep', 'ep'), 'tp', None)
    map_spec = P(None, None)

    def device_step(x_in, route_ids, gate_vals, w_gate, w_up, w_down, old_map, move_src, move_dst):
        layers, slots, width, part = w_gate.shape
        tokens, top_k = route_ids.shape[1], route_ids.shape[2]
        all_slots = group * slots
        cap = 2 * tokens * top_k // all_slots
        half = cap // 2
        feats = width // cols
        ep = lax.axis_index('ep')
        tp = lax.axis_index('tp')

        tables = []
        expert_ids = jnp.arange(EXPERTS, dtype=jnp.int32)
        slot_ids = jnp.arange(all_slots, dtype=jnp.int32)
        before = (jnp.arange(tokens)[:, None] < jnp.arange(tokens)[None, :]).astype(BF16)
        for layer in range(layers):
            ids = route_ids[layer].T
            match = ids[None, :, :] == expert_ids[:, None, None]
            taken = jnp.any(match, axis=1)
            gate = jnp.sum(jnp.where(match, gate_vals[layer].T[None], 0.0), axis=1)
            rank = jnp.dot(taken.astype(BF16), before, preferred_element_type=F32).astype(jnp.int32)
            rank = jnp.where(taken, rank, -1)
            holds = old_map[layer][None, :] == expert_ids[:, None]
            first = jnp.min(jnp.where(holds, slot_ids[None, :], all_slots - 1), axis=1)
            tables.append((rank, gate, first))

        rank, gate, first = tables[0]
        my_slots = jnp.arange(group // 2, dtype=jnp.int32) * cols + tp
        serves = first[:, None] == my_slots[None, :]
        picked = jnp.sum(jnp.where(serves[:, :, None], rank[:, None, :] + 1, 0), axis=0) - 1
        cut = (layers, slots, 2, part // 2, width)
        w_g, w_u = jnp.swapaxes(w_gate, 2, 3), jnp.swapaxes(w_up, 2, 3)
        rows, mine, other, mine1, other1 = run_front(x_in, picked, w_g.reshape(cut), w_u.reshape(cut), w_down.reshape(cut), group, cols, cap, 0)

        pieces = group // layers
        depth = 3 * part // pieces
        packed = jnp.stack([w_g, w_u, w_down], axis=2)
        cut2 = packed.reshape(layers, slots, pieces, depth, width).transpose(0, 2, 1, 3, 4).reshape(group, slots, depth, width)
        held = lax.all_to_all(cut2, 'ep', 0, 0, tiled=True).reshape(all_slots, depth, width)
        rows, mine, held = lax.optimization_barrier((rows, mine, held))
        source = jnp.arange(all_slots, dtype=jnp.int32)
        my_layer = ep // pieces
        source = source.at[move_dst[my_layer]].set(move_src[my_layer])
        held = held[source].reshape(group, slots, depth, width)

        residual = lax.dynamic_slice_in_dim(x_in, tp * feats, feats, axis=1).T
        nrank, ngate, nfirst = tables[1]
        serving = (nfirst[:, None] == slot_ids[None, :])
        by_slot = jnp.sum(jnp.where(serving[:, :, None], nrank[:, None, :] + 1, 0), axis=0) - 1
        back = run_expert(rows, mine, other, False, width, half, group, cols, 1)
        residual, rows = run_middle(first, back, rank, gate, by_slot, residual, group, cols, cap, 2)
        rows = rows.reshape(group, width, half)
        back = run_expert(rows, mine1, other1, True, width, half, group, cols, 3)
        back, held = lax.optimization_barrier((back, held))
        got = lax.all_to_all(held, 'ep', 0, 0, tiled=True)
        y_out = run_last(nfirst, back, nrank, ngate, residual, group, cols, cap, 4).reshape(width, tokens).T

        new = got.reshape(layers, pieces, slots, depth, width).transpose(0, 2, 1, 3, 4).reshape(layers, slots, 3, part, width)
        return y_out, jnp.swapaxes(new[:, :, 0], 2, 3), jnp.swapaxes(new[:, :, 1], 2, 3), new[:, :, 2]

    return jax.shard_map(device_step, mesh=mesh, in_specs=(row_spec, layer_spec, layer_spec, col_spec, col_spec, down_spec, map_spec, map_spec, map_spec), out_specs=(row_spec, col_spec, col_spec, down_spec), check_vma=False)
```

```python
import functools

import jax
import jax.numpy as jnp
from jax import lax
from jax.experimental import pallas as pl
from jax.experimental.pallas import tpu as pltpu
from jax.sharding import PartitionSpec as P

EXPERTS = 40
F32 = jnp.float32
BF16 = jnp.bfloat16
VMEM = pl.BlockSpec(memory_space=pltpu.VMEM)
SMEM = pl.BlockSpec(memory_space=pltpu.SMEM)
ANY = pl.BlockSpec(memory_space=pl.ANY)
MESH = pl.DeviceIdType.MESH
DMA = pltpu.SemaphoreType.DMA


def params(collective):
    return pltpu.CompilerParams(has_side_effects=True, collective_id=collective)


def signal_all(group, cols):
    ep, tp = lax.axis_index('ep'), lax.axis_index('tp')
    barrier = pltpu.get_barrier_semaphore()

    def tell(k, carry):
        peer = {'tp': lax.rem(tp + k // group, cols), 'ep': lax.rem(ep + lax.rem(k, group), group)}
        pl.semaphore_signal(barrier, inc=1, device_id=peer, device_id_type=MESH)
        return carry

    lax.fori_loop(1, group * cols, tell, 0)


def wait_all(group, cols):
    pl.semaphore_wait(pltpu.get_barrier_semaphore(), group * cols - 1)


def post(src, dst, to_ep, to_tp, send_sem, recv_sem):
    ep, tp = lax.axis_index('ep'), lax.axis_index('tp')
    here = jnp.logical_and(to_ep == ep, to_tp == tp)

    @pl.when(jnp.logical_not(here))
    def _():
        pltpu.make_async_remote_copy(src, dst, send_sem, recv_sem, device_id={'tp': to_tp, 'ep': to_ep}, device_id_type=MESH).start()

    @pl.when(here)
    def _():
        pltpu.make_async_copy(src, dst, recv_sem).start()


def await_bytes(ref, sem):
    pltpu.make_async_copy(ref, ref, sem).wait()


def front_kernel(group, cols, cap, x_ref, picked_ref, g_ref, u_ref, d_ref, rows_ref, mine0_ref, other0_ref, mine1_ref, other1_ref, send_ref, rsend, rrecv, wsend, wrecv, osend, orecv):
    ep, tp = lax.axis_index('ep'), lax.axis_index('tp')
    core = lax.rem(ep, 2)
    slots = g_ref.shape[1]
    half = cap // 2
    mines, others = (mine0_ref, mine1_ref), (other0_ref, other1_ref)
    signal_all(group, cols)
    row_iota = lax.broadcasted_iota(jnp.int32, (cap, x_ref.shape[0]), 0)

    def compute(i, carry):
        pick = (picked_ref[pl.ds(i, 1), :] == row_iota).astype(BF16)
        rows = jnp.dot(pick, x_ref[...], preferred_element_type=F32).astype(BF16)
        send_ref[2 * i] = rows[:half]
        send_ref[2 * i + 1] = rows[half:]
        return carry

    lax.fori_loop(0, group // 2, compute, 0)
    wait_all(group, cols)

    def weights(layer):
        def one(k, carry):
            slot = lax.rem(tp + k // 2, slots)
            part = lax.rem(k, 2)
            for mat, ref in enumerate((g_ref, u_ref, d_ref)):
                post(ref.at[layer, slot, part], mines[layer].at[tp, mat], ep - core + part, slots * core + slot, wsend.at[layer], wrecv.at[layer])
            return carry

        lax.fori_loop(0, 2 * slots, one, 0)

    def rows(k, carry):
        to = lax.rem(ep + k, group)
        post(send_ref.at[to], rows_ref.at[ep], to, tp, rsend, rrecv)
        return carry

    weights(0)
    lax.fori_loop(0, group, rows, 0)
    weights(1)
    swaps = []
    for layer in range(2):
        await_bytes(mines[layer], wrecv.at[layer])
        swap = pltpu.make_async_remote_copy(mines[layer], others[layer], osend.at[layer], orecv.at[layer], device_id={'ep': ep + 1 - 2 * core}, device_id_type=MESH)
        swap.start()
        swaps.append(swap)
    await_bytes(rows_ref, rrecv)
    await_bytes(rows_ref.at[pl.ds(0, group - 1)], rsend)
    own = tp // slots == core
    for layer in range(2):
        @pl.when(own)
        def _():
            await_bytes(mines[layer].at[pl.ds(0, 2 * slots - 1)], wsend.at[layer])

        @pl.when(jnp.logical_not(own))
        def _():
            await_bytes(mines[layer], wsend.at[layer])

        swaps[layer].wait()


def run_front(x, picked, gates, ups, downs, group, cols, cap, collective):
    _, slots, _, part, width = gates.shape
    piece = jax.ShapeDtypeStruct((cols, 3, part, width), BF16)
    rows = (group, cap // 2, width)
    return pl.pallas_call(
        functools.partial(front_kernel, group, cols, cap),
        out_shape=(jax.ShapeDtypeStruct(rows, BF16),) + (piece,) * 4,
        in_specs=[VMEM] * 2 + [ANY] * 3,
        out_specs=(ANY,) * 5,
        scratch_shapes=[pltpu.VMEM(rows, BF16), DMA, DMA] + [DMA((2,))] * 4,
        compiler_params=params(collective),
        cost_estimate=pl.CostEstimate(flops=0, bytes_accessed=240 << 20, transcendentals=0),
    )(x, picked, gates, ups, downs)


def layers_kernel(group, cols, side, cap, source_ref, rows0_ref, mine0_ref, other0_ref, rank0_ref, gate0_ref, rank1_ref, gate1_ref, res_ref, mine1_hbm, other1_hbm, held_hbm,
                  dst_ref, got_ref, out_ref, send_ref, down_ref, back0_ref, rows1_ref, back1_ref, acc_ref, hid_ref, mine1_ref, other1_ref, held_ref, moves_ref,
                  load_sem, own_sem, osend, orecv, msend, mrecv, gsend, grecv):
    ep, tp = lax.axis_index('ep'), lax.axis_index('tp')
    me = ep * cols + tp
    core = lax.rem(ep, 2)
    here = ep // 2
    planes = group // 2
    width = mine0_ref.shape[3]
    ffn_half = mine0_ref.shape[0] * mine0_ref.shape[2]
    feats, half = out_ref.shape[1:]
    tokens = rank0_ref.shape[1]
    all_slots = rank0_ref.shape[0]
    signal_all(group, cols)
    loads = [pltpu.make_async_copy(a, b, load_sem.at[k]) for k, (a, b) in enumerate(((held_hbm, held_ref), (mine1_hbm, mine1_ref), (other1_hbm, other1_ref)))]
    for load in loads:
        load.start()

    def near(i):
        hop = jnp.where(i == 0, 1, jnp.where(i == 1, planes - 1, jnp.where(i == 2, 2, 0)))
        return lax.rem(here + hop, planes)

    def take_plane(ref, sem, i):
        plane = near(i)
        await_bytes(ref.at[pl.ds(2 * cols * plane, 2 * cols)], sem.at[plane])

    def permute(k, carry):
        moves_ref[k] = held_ref[source_ref[k]]
        return carry

    def send_moves(hop, to_core):
        to = 2 * lax.rem(here + hop, planes) + to_core
        per = all_slots // group
        post(moves_ref.at[pl.ds(to * per, per)], got_ref.at[pl.ds(ep * per, per)], to, tp, msend, mrecv)

    def experts(wide, rows_ref, mine_ref, other_ref, dest_ref, stage, first_send):
        def whole(k):
            return jnp.concatenate([mine_ref[:, k].reshape(ffn_half, width), other_ref[:, k].reshape(ffn_half, width)], axis=0)

        def pair(i):
            return 2 * near(2 * (i // 2)) + lax.rem(i, 2), 2 * near(2 * (i // 2) + 1) + lax.rem(i, 2)

        def compute(i):
            one, two = pair(i)
            if wide:
                rows = jnp.concatenate([rows_ref[pl.ds(one * cols, cols)].reshape(width, half), rows_ref[pl.ds(two * cols, cols)].reshape(width, half)], axis=1)
            else:
                rows = jnp.concatenate([rows_ref[one], rows_ref[two]], axis=0)
            dims = (((1,), (0 if wide else 1,)), ((), ()))
            gate = lax.dot_general(whole(0), rows, dims, preferred_element_type=F32)
            up = lax.dot_general(whole(1), rows, dims, preferred_element_type=F32)
            act = (jax.nn.silu(gate) * up).astype(BF16)
            out = jnp.dot(down_ref[...], act, preferred_element_type=F32).astype(BF16)
            out_ref[pl.ds(one * cols, cols)] = out[:, :half].reshape(cols, feats, half)
            out_ref[pl.ds(two * cols, cols)] = out[:, half:].reshape(cols, feats, half)

        def send(i):
            one, two = pair(i)

            def each(k, carry):
                to_ep = jnp.where(lax.rem(k, 2) == 0, one, two)
                to_tp = lax.rem(tp + k // 2, cols)
                post(out_ref.at[to_ep * cols + to_tp], dest_ref.at[me], to_ep, to_tp, osend.at[stage], orecv.at[stage, here])
                return carry

            lax.fori_loop(0, 2 * cols, each, 0)

        down_ref[...] = whole(2).T
        if wide:
            take_plane(rows_ref, orecv.at[1], 0)
            take_plane(rows_ref, orecv.at[1], 1)
        compute(0)
        first_send()
        compute(1)
        send(0)
        if wide:
            take_plane(rows_ref, orecv.at[1], 2)
            take_plane(rows_ref, orecv.at[1], 3)
        compute(2)
        send(1)
        compute(3)
        send(2)
        send(3)

    row_iota = lax.broadcasted_iota(jnp.int32, (cap, tokens), 0)

    def combine(back_ref, rank_ref, gate_ref, stage):
        for i in range(planes):
            take_plane(back_ref, orecv.at[stage], i)
            plane = near(i)

            def step(column, carry):
                block = 2 * plane * cols + column
                slot = plane * cols + column
                rows = jnp.concatenate([back_ref[block], back_ref[block + cols]], axis=1)
                pick = (rank_ref[pl.ds(slot, 1), :] == row_iota).astype(BF16)
                chosen = jnp.dot(rows, pick, preferred_element_type=F32)
                acc_ref[...] += gate_ref[pl.ds(slot, 1), :] * chosen
                return carry

            lax.fori_loop(0, cols, step, 0)
        hid_ref[...] = acc_ref[...].astype(BF16)

    everything = pl.ds(0, group * cols - 1)

    acc_ref[...] = res_ref[...].astype(F32)
    loads[0].wait()
    lax.fori_loop(0, all_slots, permute, 0)

    def first_send():
        wait_all(group, cols)
        send_moves(1, 0)
        send_moves(planes - 1, 0)

    experts(False, rows0_ref, mine0_ref, other0_ref, back0_ref, 0, first_send)
    combine(back0_ref, rank0_ref, gate0_ref, 0)
    await_bytes(back0_ref.at[everything], osend.at[0])
    send_moves(1, 1)
    send_moves(planes - 1, 1)

    def place(i):
        plane = near(2 * (i // (2 * cols)) + lax.rem(i, 2))
        return plane, lax.rem(tp + lax.rem(i, 2 * cols) // 2, cols)

    def choose(i):
        plane, column = place(i)
        pick = (rank1_ref[pl.ds(plane * cols + column, 1), :] == row_iota).astype(BF16)
        rows = lax.dot_general(hid_ref[...], pick, (((1,), (1,)), ((), ())), preferred_element_type=F32).astype(BF16)
        block = 2 * plane * cols + column
        send_ref[block] = rows[:, :half]
        send_ref[block + cols] = rows[:, half:]

    def ship(i):
        plane, column = place(i)
        block = 2 * plane * cols + column
        post(send_ref.at[block], rows1_ref.at[me], 2 * plane, column, osend.at[1], orecv.at[1, here])
        post(send_ref.at[block + cols], rows1_ref.at[me], 2 * plane + 1, column, osend.at[1], orecv.at[1, here])

    choose(0)

    def step(i, carry):
        choose(i)
        ship(i - 1)
        return carry

    lax.fori_loop(1, all_slots, step, 0)
    loads[1].wait()
    loads[2].wait()
    ship(all_slots - 1)
    acc_ref[...] = hid_ref[...].astype(F32)
    experts(True, rows1_ref, mine1_ref, other1_ref, back1_ref, 2, lambda: None)
    for to_core in range(2):
        send_moves(2, to_core)
        send_moves(0, to_core)
    combine(back1_ref, rank1_ref, gate1_ref, 2)

    z, y = tp // side, lax.rem(tp, side)
    cut = feats // 2
    low, high = pl.ds(0, cut), pl.ds(cut, cut)
    await_bytes(back0_ref.at[everything], osend.at[1])
    await_bytes(back0_ref.at[everything], osend.at[2])
    own = pltpu.make_async_copy(hid_ref, dst_ref.at[z, y], own_sem)
    own.start()
    own.wait()

    def push(ref, to_z, to_y, k):
        pltpu.make_async_remote_copy(ref, ref, gsend.at[k], grecv.at[k], device_id={'tp': to_z * side + to_y}, device_id_type=MESH).start()

    for j in range(1, side):
        push(dst_ref.at[z, y, low], z, lax.rem(y + j, side), 0)
        push(dst_ref.at[z, y, high], lax.rem(z + j, side), y, 1)
    some = pl.ds(0, side - 1)
    await_bytes(dst_ref.at[z, some, low], grecv.at[0])
    for j in range(1, side):
        push(dst_ref.at[z, :, low], lax.rem(z + j, side), y, 2)
    await_bytes(dst_ref.at[some, y, high], grecv.at[1])
    for j in range(1, side):
        push(dst_ref.at[:, y, high], z, lax.rem(y + j, side), 3)
    await_bytes(dst_ref.at[some, :, low], grecv.at[2])
    await_bytes(dst_ref.at[:, some, high], grecv.at[3])
    await_bytes(dst_ref.at[z, some, low], gsend.at[0])
    await_bytes(dst_ref.at[some, y, high], gsend.at[1])
    await_bytes(dst_ref.at[some, :, low], gsend.at[2])
    await_bytes(dst_ref.at[:, some, high], gsend.at[3])
    await_bytes(got_ref, mrecv)
    await_bytes(got_ref.at[pl.ds(0, all_slots - all_slots // group)], msend)


def run_layers(source, rows, w0, tables, residual, w1, held, group, cols, cap, collective):
    feats, tokens = residual.shape
    side = int(round(cols ** 0.5))
    piece = w0[0].shape
    width = piece[3]
    ffn = 2 * piece[0] * piece[2]
    blocks = pltpu.VMEM((group * cols, feats, cap // 2), BF16)
    return pl.pallas_call(
        functools.partial(layers_kernel, group, cols, side, cap),
        out_shape=(jax.ShapeDtypeStruct((side, side, feats, tokens), BF16), jax.ShapeDtypeStruct(held.shape, BF16)),
        in_specs=[SMEM] + [VMEM] * 8 + [ANY] * 3,
        out_specs=(ANY, ANY),
        scratch_shapes=[blocks, blocks, pltpu.VMEM((width, ffn), BF16), blocks, blocks, blocks, pltpu.VMEM((feats, tokens), F32), pltpu.VMEM((feats, tokens), BF16),
                        pltpu.VMEM(piece, BF16), pltpu.VMEM(piece, BF16), pltpu.VMEM(held.shape, BF16), pltpu.VMEM(held.shape, BF16),
                        DMA((3,)), DMA, DMA((3,)), DMA((3, group // 2)), DMA, DMA, DMA((4,)), DMA((4,))],
        compiler_params=pltpu.CompilerParams(has_side_effects=True, collective_id=collective, vmem_limit_bytes=60 << 20),
        cost_estimate=pl.CostEstimate(flops=40 << 30, bytes_accessed=480 << 20, transcendentals=0),
    )(source, rows, *w0, *tables, residual, *w1, held)


def solution(mesh):
    group = mesh.shape['ep']
    cols = mesh.shape['tp']
    row_spec = P(('rep', 'ep'), None)
    layer_spec = P(None, ('rep', 'ep'), None)
    col_spec = P(None, ('rep', 'ep'), None, 'tp')
    down_spec = P(None, ('rep', 'ep'), 'tp', None)
    map_spec = P(None, None)

    def device_step(x_in, route_ids, gate_vals, w_gate, w_up, w_down, old_map, move_src, move_dst):
        layers, slots, width, part = w_gate.shape
        tokens, top_k = route_ids.shape[1], route_ids.shape[2]
        all_slots = group * slots
        cap = 2 * tokens * top_k // all_slots
        half = cap // 2
        feats = width // cols
        ep = lax.axis_index('ep')
        tp = lax.axis_index('tp')

        tables = []
        expert_ids = jnp.arange(EXPERTS, dtype=jnp.int32)
        slot_ids = jnp.arange(all_slots, dtype=jnp.int32)
        before = (jnp.arange(tokens)[:, None] < jnp.arange(tokens)[None, :]).astype(BF16)
        for layer in range(layers):
            ids = route_ids[layer].T
            match = ids[None, :, :] == expert_ids[:, None, None]
            taken = jnp.any(match, axis=1)
            gate = jnp.sum(jnp.where(match, gate_vals[layer].T[None], 0.0), axis=1)
            rank = jnp.dot(taken.astype(BF16), before, preferred_element_type=F32).astype(jnp.int32)
            rank = jnp.where(taken, rank, -1)
            holds = old_map[layer][None, :] == expert_ids[:, None]
            first = jnp.min(jnp.where(holds, slot_ids[None, :], all_slots - 1), axis=1)
            serving = (first[:, None] == slot_ids[None, :])[:, :, None]
            by_slot = jnp.sum(jnp.where(serving, rank[:, None, :] + 1, 0), axis=0) - 1
            gate_slot = jnp.sum(jnp.where(serving, gate[:, None, :], 0.0), axis=0)
            tables.append((by_slot, gate_slot, rank, first))

        _, _, rank, first = tables[0]
        my_slots = jnp.arange(group // 2, dtype=jnp.int32) * cols + tp
        serves = first[:, None] == my_slots[None, :]
        picked = jnp.sum(jnp.where(serves[:, :, None], rank[:, None, :] + 1, 0), axis=0) - 1
        cut = (layers, slots, 2, part // 2, width)
        w_g, w_u = jnp.swapaxes(w_gate, 2, 3), jnp.swapaxes(w_up, 2, 3)
        rows, mine, other, mine1, other1 = run_front(x_in, picked, w_g.reshape(cut), w_u.reshape(cut), w_down.reshape(cut), group, cols, cap, 0)

        pieces = group // layers
        depth = 3 * part // pieces
        packed = jnp.stack([w_g, w_u, w_down], axis=2)
        cut2 = packed.reshape(layers, slots, pieces, depth, width).transpose(0, 2, 1, 3, 4).reshape(group, slots, depth, width)
        held = lax.all_to_all(cut2, 'ep', 0, 0, tiled=True).reshape(all_slots, depth, width)
        source = jnp.arange(all_slots, dtype=jnp.int32)
        my_layer = ep // pieces
        source = source.at[move_dst[my_layer]].set(move_src[my_layer])
        residual = lax.dynamic_slice_in_dim(x_in, tp * feats, feats, axis=1).T
        y_out, got = run_layers(source, rows, (mine, other), tables[0][:2] + tables[1][:2], residual, (mine1, other1), held, group, cols, cap, 1)
        y_out = y_out.reshape(width, tokens).T

        new = got.reshape(layers, pieces, slots, depth, width).transpose(0, 2, 1, 3, 4).reshape(layers, slots, 3, part, width)
        return y_out, jnp.swapaxes(new[:, :, 0], 2, 3), jnp.swapaxes(new[:, :, 1], 2, 3), new[:, :, 2]

    return jax.shard_map(device_step, mesh=mesh, in_specs=(row_spec, layer_spec, layer_spec, col_spec, col_spec, down_spec, map_spec, map_spec, map_spec), out_specs=(row_spec, col_spec, col_spec, down_spec), check_vma=False)
```

```python
import functools

import jax
import jax.numpy as jnp
from jax import lax
from jax.experimental import pallas as pl
from jax.experimental.pallas import tpu as pltpu
from jax.sharding import PartitionSpec as P

EXPERTS = 40
F32 = jnp.float32
BF16 = jnp.bfloat16
VMEM = pl.BlockSpec(memory_space=pltpu.VMEM)
SMEM = pl.BlockSpec(memory_space=pltpu.SMEM)
ANY = pl.BlockSpec(memory_space=pl.ANY)
MESH = pl.DeviceIdType.MESH
DMA = pltpu.SemaphoreType.DMA


def params(collective):
    return pltpu.CompilerParams(has_side_effects=True, collective_id=collective)


def signal_all(group, cols):
    ep, tp = lax.axis_index('ep'), lax.axis_index('tp')
    barrier = pltpu.get_barrier_semaphore()

    def tell(k, carry):
        peer = {'tp': lax.rem(tp + k // group, cols), 'ep': lax.rem(ep + lax.rem(k, group), group)}
        pl.semaphore_signal(barrier, inc=1, device_id=peer, device_id_type=MESH)
        return carry

    lax.fori_loop(1, group * cols, tell, 0)


def wait_all(group, cols):
    pl.semaphore_wait(pltpu.get_barrier_semaphore(), group * cols - 1)


def post(src, dst, to_ep, to_tp, send_sem, recv_sem):
    ep, tp = lax.axis_index('ep'), lax.axis_index('tp')
    here = jnp.logical_and(to_ep == ep, to_tp == tp)

    @pl.when(jnp.logical_not(here))
    def _():
        pltpu.make_async_remote_copy(src, dst, send_sem, recv_sem, device_id={'tp': to_tp, 'ep': to_ep}, device_id_type=MESH).start()

    @pl.when(here)
    def _():
        pltpu.make_async_copy(src, dst, recv_sem).start()


def await_bytes(ref, sem):
    pltpu.make_async_copy(ref, ref, sem).wait()


def layers_kernel(group, cols, side, cap, source_ref, sexp_ref, ids_ref, gates_ref, x_ref, res_ref, g16, u16, d16, g8, u8, d8,
                  dst_ref, newg_ref, newu_ref, newd_ref, rank0_ref, gate0_ref, rank1_ref, gate1_ref, rsend_ref, rows0_ref, mine0_ref, other0_ref, mine1_ref, other1_ref,
                  out_ref, send_ref, down_ref, back0_ref, rows1_ref, back1_ref, acc_ref, hid_ref, held_ref, moves_ref,
                  own_sem, rsend, rrecv, wsend, wrecv, ssend, srecv, hsend, hrecv, msend, mrecv, osend, orecv, gsend, grecv):
    ep, tp = lax.axis_index('ep'), lax.axis_index('tp')
    me = ep * cols + tp
    core = lax.rem(ep, 2)
    here = ep // 2
    planes = group // 2
    width = mine0_ref.shape[3]
    ffn_half = mine0_ref.shape[0] * mine0_ref.shape[2]
    feats, half = out_ref.shape[1:]
    all_slots, tokens = rank0_ref.shape
    slots = all_slots // group
    pieces = group // 2
    signal_all(group, cols)
    def near(i):
        hop = jnp.where(i == 0, 1, jnp.where(i == 1, planes - 1, jnp.where(i == 2, 2, 0)))
        return lax.rem(here + hop, planes)

    def take_plane(ref, sem, i):
        plane = near(i)
        per = ref.shape[0] // planes
        await_bytes(ref.at[pl.ds(per * plane, per)], sem.at[plane])

    row_iota = lax.broadcasted_iota(jnp.int32, (cap, tokens), 0)

    def table(layer, rank_ref, gate_ref):
        holds = sexp_ref[layer]
        taken = jnp.zeros((all_slots, tokens), F32)
        gate = jnp.zeros((all_slots, tokens), F32)
        for j in range(ids_ref.shape[1]):
            match = ids_ref[layer, j:j + 1, :] == holds
            taken = jnp.where(match, 1.0, taken)
            gate = jnp.where(match, gates_ref[layer, j:j + 1, :], gate)
        earlier = lax.broadcasted_iota(jnp.int32, (tokens, tokens), 0) < lax.broadcasted_iota(jnp.int32, (tokens, tokens), 1)
        rank = jnp.dot(taken.astype(BF16), earlier.astype(BF16), preferred_element_type=F32).astype(jnp.int32)
        rank_ref[...] = jnp.where(taken > 0.0, rank, -1)
        gate_ref[...] = gate

    def first_rows(i, carry):
        pick = (rank0_ref[pl.ds(i * cols + tp, 1), :] == row_iota).astype(BF16)
        rows = jnp.dot(pick, x_ref[...], preferred_element_type=F32).astype(BF16)
        rsend_ref[2 * i] = rows[:half]
        rsend_ref[2 * i + 1] = rows[half:]
        return carry

    def send_weights(layer, mine_ref):
        def one(k, carry):
            slot = lax.rem(tp + k // 2, slots)
            part = lax.rem(k, 2)
            for mat, ref in enumerate((g16, u16, d16)):
                post(ref.at[layer, slot, part], mine_ref.at[tp, mat], ep - core + part, slots * core + slot, wsend.at[layer], wrecv.at[layer])
            return carry

        lax.fori_loop(0, 2 * slots, one, 0)

    def swap_weights(layer, mine_ref, other_ref):
        await_bytes(mine_ref, wrecv.at[layer])
        swap = pltpu.make_async_remote_copy(mine_ref, other_ref, ssend.at[layer], srecv.at[layer], device_id={'ep': ep + 1 - 2 * core}, device_id_type=MESH)
        swap.start()
        return swap

    def send_rows(k, carry):
        to = 2 * near(k // 2) + lax.rem(k, 2)
        post(rsend_ref.at[to], rows0_ref.at[ep], to, tp, rsend, rrecv.at[here])
        return carry

    def gather_moves(k, carry):
        to = 2 * near(k // 2) + lax.rem(k, 2)
        for mat, ref in enumerate((g8, u8, d8)):
            post(ref.at[to // pieces, :, lax.rem(to, pieces)], held_ref.at[pl.ds(ep * slots, slots), mat], to, tp, hsend, hrecv)
        return carry

    def permute(k, carry):
        moves_ref[k] = held_ref[source_ref[k]]
        return carry

    def send_moves(i, to_core):
        to = 2 * near(i) + to_core
        for mat, ref in enumerate((newg_ref, newu_ref, newd_ref)):
            post(moves_ref.at[pl.ds(to * slots, slots), mat], ref.at[ep // pieces, :, lax.rem(ep, pieces)], to, tp, msend.at[mat], mrecv.at[mat])

    def experts(wide, rows_ref, mine_ref, other_ref, dest_ref, stage):
        def whole(k):
            return jnp.concatenate([mine_ref[:, k].reshape(ffn_half, width), other_ref[:, k].reshape(ffn_half, width)], axis=0)

        def pair(i):
            return 2 * near(2 * (i // 2)) + lax.rem(i, 2), 2 * near(2 * (i // 2) + 1) + lax.rem(i, 2)

        def compute(i):
            one, two = pair(i)
            if wide:
                rows = jnp.concatenate([rows_ref[pl.ds(one * cols, cols)].reshape(width, half), rows_ref[pl.ds(two * cols, cols)].reshape(width, half)], axis=1)
            else:
                rows = jnp.concatenate([rows_ref[one], rows_ref[two]], axis=0)
            dims = (((1,), (0 if wide else 1,)), ((), ()))
            gate = lax.dot_general(whole(0), rows, dims, preferred_element_type=F32)
            up = lax.dot_general(whole(1), rows, dims, preferred_element_type=F32)
            act = (jax.nn.silu(gate) * up).astype(BF16)
            out = jnp.dot(down_ref[...], act, preferred_element_type=F32).astype(BF16)
            out_ref[pl.ds(one * cols, cols)] = out[:, :half].reshape(cols, feats, half)
            out_ref[pl.ds(two * cols, cols)] = out[:, half:].reshape(cols, feats, half)

        def send(i):
            one, two = pair(i)

            def each(k, carry):
                to_ep = jnp.where(lax.rem(k, 2) == 0, one, two)
                to_tp = lax.rem(tp + k // 2, cols)
                post(out_ref.at[to_ep * cols + to_tp], dest_ref.at[me], to_ep, to_tp, osend.at[stage], orecv.at[stage, here])
                return carry

            lax.fori_loop(0, 2 * cols, each, 0)

        down_ref[...] = whole(2).T
        arrived = orecv.at[1] if wide else rrecv
        take_plane(rows_ref, arrived, 0)
        take_plane(rows_ref, arrived, 1)
        compute(0)
        compute(1)
        send(0)
        take_plane(rows_ref, arrived, 2)
        take_plane(rows_ref, arrived, 3)
        compute(2)
        send(1)
        compute(3)
        send(2)
        send(3)

    def combine(back_ref, rank_ref, gate_ref, stage):
        for i in range(planes):
            take_plane(back_ref, orecv.at[stage], i)
            plane = near(i)

            def step(column, carry):
                block = 2 * plane * cols + column
                slot = plane * cols + column
                rows = jnp.concatenate([back_ref[block], back_ref[block + cols]], axis=1)
                pick = (rank_ref[pl.ds(slot, 1), :] == row_iota).astype(BF16)
                chosen = jnp.dot(rows, pick, preferred_element_type=F32)
                acc_ref[...] += gate_ref[pl.ds(slot, 1), :] * chosen
                return carry

            lax.fori_loop(0, cols, step, 0)
        hid_ref[...] = acc_ref[...].astype(BF16)

    everything = pl.ds(0, group * cols - 1)

    table(0, rank0_ref, gate0_ref)
    lax.fori_loop(0, planes, first_rows, 0)
    wait_all(group, cols)
    send_weights(0, mine0_ref)
    lax.fori_loop(0, group, send_rows, 0)
    send_weights(1, mine1_ref)
    lax.fori_loop(0, group, gather_moves, 0)
    table(1, rank1_ref, gate1_ref)
    acc_ref[...] = res_ref[...].astype(F32)
    swap0 = swap_weights(0, mine0_ref, other0_ref)
    swap0.wait_recv()
    experts(False, rows0_ref, mine0_ref, other0_ref, back0_ref, 0)
    swap1 = swap_weights(1, mine1_ref, other1_ref)
    combine(back0_ref, rank0_ref, gate0_ref, 0)
    await_bytes(back0_ref.at[everything], osend.at[0])
    await_bytes(held_ref, hrecv)
    lax.fori_loop(0, all_slots, permute, 0)

    def place(i):
        plane = near(2 * (i // (2 * cols)) + lax.rem(i, 2))
        return plane, lax.rem(tp + lax.rem(i, 2 * cols) // 2, cols)

    def choose(i):
        plane, column = place(i)
        pick = (rank1_ref[pl.ds(plane * cols + column, 1), :] == row_iota).astype(BF16)
        rows = lax.dot_general(hid_ref[...], pick, (((1,), (1,)), ((), ())), preferred_element_type=F32).astype(BF16)
        block = 2 * plane * cols + column
        send_ref[block] = rows[:, :half]
        send_ref[block + cols] = rows[:, half:]

    def ship(i):
        plane, column = place(i)
        block = 2 * plane * cols + column
        post(send_ref.at[block], rows1_ref.at[me], 2 * plane, column, osend.at[1], orecv.at[1, here])
        post(send_ref.at[block + cols], rows1_ref.at[me], 2 * plane + 1, column, osend.at[1], orecv.at[1, here])

    choose(0)
    for to_core in range(2):
        send_moves(0, to_core)
        send_moves(1, to_core)

    def step(i, carry):
        choose(i)
        ship(i - 1)
        return carry

    lax.fori_loop(1, all_slots, step, 0)
    swap1.wait_recv()
    ship(all_slots - 1)
    acc_ref[...] = hid_ref[...].astype(F32)
    experts(True, rows1_ref, mine1_ref, other1_ref, back1_ref, 2)
    for to_core in range(2):
        send_moves(2, to_core)
        send_moves(3, to_core)
    combine(back1_ref, rank1_ref, gate1_ref, 2)

    z, y = tp // side, lax.rem(tp, side)
    cut = feats // 2
    low, high = pl.ds(0, cut), pl.ds(cut, cut)
    await_bytes(back0_ref.at[everything], osend.at[1])
    await_bytes(back0_ref.at[everything], osend.at[2])
    own = pltpu.make_async_copy(hid_ref, dst_ref.at[z, y], own_sem)
    own.start()
    own.wait()

    def push(ref, to_z, to_y, k):
        pltpu.make_async_remote_copy(ref, ref, gsend.at[k], grecv.at[k], device_id={'tp': to_z * side + to_y}, device_id_type=MESH).start()

    for j in range(1, side):
        push(dst_ref.at[z, y, low], z, lax.rem(y + j, side), 0)
        push(dst_ref.at[z, y, high], lax.rem(z + j, side), y, 1)
    some = pl.ds(0, side - 1)
    await_bytes(dst_ref.at[z, some, low], grecv.at[0])
    for j in range(1, side):
        push(dst_ref.at[z, :, low], lax.rem(z + j, side), y, 2)
    await_bytes(dst_ref.at[some, y, high], grecv.at[1])
    for j in range(1, side):
        push(dst_ref.at[:, y, high], z, lax.rem(y + j, side), 3)
    await_bytes(dst_ref.at[some, :, low], grecv.at[2])
    await_bytes(dst_ref.at[:, some, high], grecv.at[3])
    await_bytes(dst_ref.at[z, some, low], gsend.at[0])
    await_bytes(dst_ref.at[some, y, high], gsend.at[1])
    await_bytes(dst_ref.at[some, :, low], gsend.at[2])
    await_bytes(dst_ref.at[:, some, high], gsend.at[3])
    sent = pl.ds(0, all_slots - slots)
    for mat, ref in enumerate((newg_ref, newu_ref, newd_ref)):
        await_bytes(ref, mrecv.at[mat])
        await_bytes(held_ref.at[sent, mat], msend.at[mat])
    await_bytes(held_ref.at[sent], hsend)
    await_bytes(rows0_ref.at[pl.ds(0, group - 1)], rsend)
    own_slot = tp // slots == core
    for layer, (mine_ref, swap) in enumerate(((mine0_ref, swap0), (mine1_ref, swap1))):
        swap.wait_send()

        @pl.when(own_slot)
        def _():
            await_bytes(mine_ref.at[pl.ds(0, cols - 1)], wsend.at[layer])

        @pl.when(jnp.logical_not(own_slot))
        def _():
            await_bytes(mine_ref, wsend.at[layer])


def run_layers(source, holds, ids, gates, x, residual, halves, pieces, group, cols, cap):
    feats, tokens = residual.shape
    width = x.shape[1]
    side = int(round(cols ** 0.5))
    _, slots, _, part, _ = halves[0].shape
    depth = pieces[0].shape[3]
    all_slots = group * slots
    half = cap // 2
    ffn = 2 * cols * part

    def vmem(*shape, dtype=BF16):
        return pltpu.VMEM(shape, dtype)

    weights = vmem(cols, 3, part, width)
    blocks = vmem(group * cols, feats, half)
    rows = vmem(group, half, width)
    held = vmem(all_slots, 3, depth, width)
    return pl.pallas_call(
        functools.partial(layers_kernel, group, cols, side, cap),
        out_shape=(jax.ShapeDtypeStruct((side, side, feats, tokens), BF16),) + (jax.ShapeDtypeStruct(pieces[0].shape, BF16),) * 3,
        in_specs=[SMEM] + [VMEM] * 5 + [ANY] * 6,
        out_specs=(ANY,) * 4,
        scratch_shapes=[vmem(all_slots, tokens, dtype=jnp.int32), vmem(all_slots, tokens, dtype=F32)] * 2 + [rows, rows] + [weights] * 4
                       + [blocks, blocks, vmem(width, ffn), blocks, blocks, blocks, vmem(feats, tokens, dtype=F32), vmem(feats, tokens), held, held,
                          DMA, DMA, DMA((group // 2,)), DMA((2,)), DMA((2,)), DMA((2,)), DMA((2,)), DMA, DMA, DMA((3,)), DMA((3,)), DMA((3,)), DMA((3, group // 2)), DMA((4,)), DMA((4,))],
        compiler_params=pltpu.CompilerParams(has_side_effects=True, collective_id=0, vmem_limit_bytes=62 << 20),
    )(source, holds, ids, gates, x, residual, *halves, *pieces)


def solution(mesh):
    group = mesh.shape['ep']
    cols = mesh.shape['tp']
    row_spec = P(('rep', 'ep'), None)
    layer_spec = P(None, ('rep', 'ep'), None)
    col_spec = P(None, ('rep', 'ep'), None, 'tp')
    down_spec = P(None, ('rep', 'ep'), 'tp', None)
    map_spec = P(None, None)

    def device_step(x_in, route_ids, gate_vals, w_gate, w_up, w_down, old_map, move_src, move_dst):
        layers, slots, width, part = w_gate.shape
        tokens, top_k = route_ids.shape[1], route_ids.shape[2]
        all_slots = group * slots
        cap = 2 * tokens * top_k // all_slots
        half = cap // 2
        feats = width // cols
        ep = lax.axis_index('ep')
        tp = lax.axis_index('tp')

        slot_ids = jnp.arange(all_slots, dtype=jnp.int32)
        again = (old_map[:, :, None] == old_map[:, None, :]) & (slot_ids[None, :] < slot_ids[:, None])[None]
        holds = jnp.where(jnp.any(again, axis=2), -1, old_map)[:, :, None]

        pieces = group // layers
        mine = ep // pieces
        hit = slot_ids[:, None] == move_dst[mine][None, :]
        source = jnp.where(jnp.any(hit, axis=1), jnp.sum(jnp.where(hit, move_src[mine][None, :], 0), axis=1), slot_ids)

        residual = lax.dynamic_slice_in_dim(x_in, tp * feats, feats, axis=1).T
        mats = (jnp.swapaxes(w_gate, 2, 3), jnp.swapaxes(w_up, 2, 3), w_down)
        halves = [m.reshape(layers, slots, 2, part // 2, width) for m in mats]
        groups = [m.reshape(layers, slots, pieces, part // pieces, width) for m in mats]
        y_out, *new = run_layers(source, holds, jnp.swapaxes(route_ids, 1, 2), jnp.swapaxes(gate_vals, 1, 2), x_in, residual, halves, groups, group, cols, cap)
        y_out = y_out.reshape(width, tokens).T
        new = [m.reshape(layers, slots, part, width) for m in new]
        return y_out, jnp.swapaxes(new[0], 2, 3), jnp.swapaxes(new[1], 2, 3), new[2]

    return jax.shard_map(device_step, mesh=mesh, in_specs=(row_spec, layer_spec, layer_spec, col_spec, col_spec, down_spec, map_spec, map_spec, map_spec), out_specs=(row_spec, col_spec, col_spec, down_spec), check_vma=False)
```

```python
import functools

import jax
import jax.numpy as jnp
from jax import lax
from jax.experimental import pallas as pl
from jax.experimental.pallas import tpu as pltpu
from jax.sharding import PartitionSpec as P

EXPERTS = 40
F32 = jnp.float32
BF16 = jnp.bfloat16
VMEM = pl.BlockSpec(memory_space=pltpu.VMEM)
SMEM = pl.BlockSpec(memory_space=pltpu.SMEM)
ANY = pl.BlockSpec(memory_space=pl.ANY)
MESH = pl.DeviceIdType.MESH
DMA = pltpu.SemaphoreType.DMA


def params(collective):
    return pltpu.CompilerParams(has_side_effects=True, collective_id=collective)


def signal_all(group, cols):
    ep, tp = lax.axis_index('ep'), lax.axis_index('tp')
    barrier = pltpu.get_barrier_semaphore()

    def tell(k, carry):
        peer = {'tp': lax.rem(tp + k // group, cols), 'ep': lax.rem(ep + lax.rem(k, group), group)}
        pl.semaphore_signal(barrier, inc=1, device_id=peer, device_id_type=MESH)
        return carry

    lax.fori_loop(1, group * cols, tell, 0)


def wait_all(group, cols):
    pl.semaphore_wait(pltpu.get_barrier_semaphore(), group * cols - 1)


def post(src, dst, to_ep, to_tp, send_sem, recv_sem):
    ep, tp = lax.axis_index('ep'), lax.axis_index('tp')
    here = jnp.logical_and(to_ep == ep, to_tp == tp)

    @pl.when(jnp.logical_not(here))
    def _():
        pltpu.make_async_remote_copy(src, dst, send_sem, recv_sem, device_id={'tp': to_tp, 'ep': to_ep}, device_id_type=MESH).start()

    @pl.when(here)
    def _():
        pltpu.make_async_copy(src, dst, recv_sem).start()


def await_bytes(ref, sem):
    pltpu.make_async_copy(ref, ref, sem).wait()


def layers_kernel(group, cols, side, cap, source_ref, sexp_ref, ids_ref, gates_ref, x_ref, res_ref, g16, u16, d16, g8, u8, d8,
                  dst_ref, newg_ref, newu_ref, newd_ref, rank0_ref, gate0_ref, rank1_ref, gate1_ref, rsend_ref, rows0_ref, mine0_ref, other0_ref, mine1_ref, other1_ref,
                  out_ref, send_ref, down_ref, back0_ref, rows1_ref, back1_ref, acc_ref, hid_ref, held_ref, moves_ref,
                  own_sem, rsend, rrecv, wsend, wrecv, ssend, srecv, hsend, hrecv, msend, mrecv, osend, orecv, gsend, grecv):
    ep, tp = lax.axis_index('ep'), lax.axis_index('tp')
    me = ep * cols + tp
    core = lax.rem(ep, 2)
    here = ep // 2
    planes = group // 2
    width = mine0_ref.shape[3]
    ffn_half = mine0_ref.shape[0] * mine0_ref.shape[2]
    feats, half = out_ref.shape[1:]
    all_slots, tokens = rank0_ref.shape
    slots = all_slots // group
    pieces = group // 2
    signal_all(group, cols)
    def near(i):
        hop = jnp.where(i == 0, 1, jnp.where(i == 1, planes - 1, jnp.where(i == 2, 2, 0)))
        return lax.rem(here + hop, planes)

    def take_plane(ref, sem, i):
        plane = near(i)
        per = ref.shape[0] // planes
        await_bytes(ref.at[pl.ds(per * plane, per)], sem.at[plane])

    row_iota = lax.broadcasted_iota(jnp.int32, (cap, tokens), 0)

    def table(layer, rank_ref, gate_ref):
        holds = sexp_ref[layer]
        taken = jnp.zeros((all_slots, tokens), F32)
        gate = jnp.zeros((all_slots, tokens), F32)
        for j in range(ids_ref.shape[1]):
            match = ids_ref[layer, j:j + 1, :] == holds
            taken = jnp.where(match, 1.0, taken)
            gate = jnp.where(match, gates_ref[layer, j:j + 1, :], gate)
        earlier = lax.broadcasted_iota(jnp.int32, (tokens, tokens), 0) < lax.broadcasted_iota(jnp.int32, (tokens, tokens), 1)
        rank = jnp.dot(taken.astype(BF16), earlier.astype(BF16), preferred_element_type=F32).astype(jnp.int32)
        rank_ref[...] = jnp.where(taken > 0.0, rank, -1)
        gate_ref[...] = gate

    def first_rows(i, carry):
        pick = (rank0_ref[pl.ds(i * cols + tp, 1), :] == row_iota).astype(BF16)
        rows = jnp.dot(pick, x_ref[...], preferred_element_type=F32).astype(BF16)
        rsend_ref[2 * i] = rows[:half]
        rsend_ref[2 * i + 1] = rows[half:]
        return carry

    def send_weights(layer, mine_ref):
        def one(k, carry):
            slot = lax.rem(tp + k // 2, slots)
            part = lax.rem(k, 2)
            for mat, ref in enumerate((g16, u16, d16)):
                post(ref.at[layer, slot, part], mine_ref.at[tp, mat], ep - core + part, slots * core + slot, wsend.at[layer], wrecv.at[layer])
            return carry

        lax.fori_loop(0, 2 * slots, one, 0)

    def swap_weights(layer, mine_ref, other_ref):
        await_bytes(mine_ref, wrecv.at[layer])
        swap = pltpu.make_async_remote_copy(mine_ref, other_ref, ssend.at[layer], srecv.at[layer], device_id={'ep': ep + 1 - 2 * core}, device_id_type=MESH)
        swap.start()
        return swap

    def send_rows(k, carry):
        to = 2 * near(k // 2) + lax.rem(k, 2)
        post(rsend_ref.at[to], rows0_ref.at[ep], to, tp, rsend, rrecv.at[here])
        return carry

    def gather_moves(k, carry):
        to = 2 * near(k // 2) + lax.rem(k, 2)
        for mat, ref in enumerate((g8, u8, d8)):
            post(ref.at[to // pieces, :, lax.rem(to, pieces)], held_ref.at[pl.ds(ep * slots, slots), mat], to, tp, hsend, hrecv)
        return carry

    def permute(k, carry):
        moves_ref[k] = held_ref[source_ref[k]]
        return carry

    def send_moves(i, to_core):
        to = 2 * near(i) + to_core
        for mat, ref in enumerate((newg_ref, newu_ref, newd_ref)):
            post(moves_ref.at[pl.ds(to * slots, slots), mat], ref.at[ep // pieces, :, lax.rem(ep, pieces)], to, tp, msend.at[mat], mrecv.at[mat])

    def experts(wide, rows_ref, mine_ref, other_ref, dest_ref, stage):
        def whole(k):
            return jnp.concatenate([mine_ref[:, k].reshape(ffn_half, width), other_ref[:, k].reshape(ffn_half, width)], axis=0)

        def pair(i):
            return 2 * near(2 * (i // 2)) + lax.rem(i, 2), 2 * near(2 * (i // 2) + 1) + lax.rem(i, 2)

        def compute(i):
            one, two = pair(i)
            if wide:
                rows = jnp.concatenate([rows_ref[pl.ds(one * cols, cols)].reshape(width, half), rows_ref[pl.ds(two * cols, cols)].reshape(width, half)], axis=1)
            else:
                rows = jnp.concatenate([rows_ref[one], rows_ref[two]], axis=0)
            dims = (((1,), (0 if wide else 1,)), ((), ()))
            gate = lax.dot_general(whole(0), rows, dims, preferred_element_type=F32)
            up = lax.dot_general(whole(1), rows, dims, preferred_element_type=F32)
            act = (jax.nn.silu(gate) * up).astype(BF16)
            out = jnp.dot(down_ref[...], act, preferred_element_type=F32).astype(BF16)
            out_ref[pl.ds(one * cols, cols)] = out[:, :half].reshape(cols, feats, half)
            out_ref[pl.ds(two * cols, cols)] = out[:, half:].reshape(cols, feats, half)

        def send(i):
            one, two = pair(i)

            def each(k, carry):
                to_ep = jnp.where(lax.rem(k, 2) == 0, one, two)
                to_tp = lax.rem(tp + k // 2, cols)
                post(out_ref.at[to_ep * cols + to_tp], dest_ref.at[me], to_ep, to_tp, osend.at[stage], orecv.at[stage, here])
                return carry

            lax.fori_loop(0, 2 * cols, each, 0)

        down_ref[...] = whole(2).T
        arrived = orecv.at[1] if wide else rrecv
        take_plane(rows_ref, arrived, 0)
        take_plane(rows_ref, arrived, 1)
        compute(0)
        compute(1)
        send(0)
        take_plane(rows_ref, arrived, 2)
        take_plane(rows_ref, arrived, 3)
        compute(2)
        send(1)
        compute(3)
        send(2)
        send(3)

    def combine(back_ref, rank_ref, gate_ref, stage):
        for i in range(planes):
            take_plane(back_ref, orecv.at[stage], i)
            plane = near(i)

            def step(column, carry):
                block = 2 * plane * cols + column
                slot = plane * cols + column
                rows = jnp.concatenate([back_ref[block], back_ref[block + cols]], axis=1)
                pick = (rank_ref[pl.ds(slot, 1), :] == row_iota).astype(BF16)
                chosen = jnp.dot(rows, pick, preferred_element_type=F32)
                acc_ref[...] += gate_ref[pl.ds(slot, 1), :] * chosen
                return carry

            lax.fori_loop(0, cols, step, 0)
        hid_ref[...] = acc_ref[...].astype(BF16)

    everything = pl.ds(0, group * cols - 1)

    table(0, rank0_ref, gate0_ref)
    lax.fori_loop(0, planes, first_rows, 0)
    wait_all(group, cols)
    send_weights(0, mine0_ref)
    lax.fori_loop(0, group, send_rows, 0)
    send_weights(1, mine1_ref)
    lax.fori_loop(0, group, gather_moves, 0)
    table(1, rank1_ref, gate1_ref)
    acc_ref[...] = res_ref[...].astype(F32)
    swap0 = swap_weights(0, mine0_ref, other0_ref)
    swap0.wait_recv()
    experts(False, rows0_ref, mine0_ref, other0_ref, back0_ref, 0)
    swap1 = swap_weights(1, mine1_ref, other1_ref)
    combine(back0_ref, rank0_ref, gate0_ref, 0)
    await_bytes(back0_ref.at[everything], osend.at[0])

    def place(i):
        plane = near(2 * (i // (2 * cols)) + lax.rem(i, 2))
        return plane, lax.rem(tp + lax.rem(i, 2 * cols) // 2, cols)

    def choose(i):
        plane, column = place(i)
        pick = (rank1_ref[pl.ds(plane * cols + column, 1), :] == row_iota).astype(BF16)
        rows = lax.dot_general(hid_ref[...], pick, (((1,), (1,)), ((), ())), preferred_element_type=F32).astype(BF16)
        block = 2 * plane * cols + column
        send_ref[block] = rows[:, :half]
        send_ref[block + cols] = rows[:, half:]

    def ship(i):
        plane, column = place(i)
        block = 2 * plane * cols + column
        post(send_ref.at[block], rows1_ref.at[me], 2 * plane, column, osend.at[1], orecv.at[1, here])
        post(send_ref.at[block + cols], rows1_ref.at[me], 2 * plane + 1, column, osend.at[1], orecv.at[1, here])

    choose(0)

    def step(i, carry):
        choose(i)
        ship(i - 1)
        return carry

    lax.fori_loop(1, all_slots, step, 0)
    swap1.wait_recv()
    ship(all_slots - 1)
    await_bytes(held_ref, hrecv)
    lax.fori_loop(0, all_slots, permute, 0)
    acc_ref[...] = hid_ref[...].astype(F32)
    experts(True, rows1_ref, mine1_ref, other1_ref, back1_ref, 2)
    for to_core in range(2):
        for i in range(planes):
            send_moves(i, to_core)
    combine(back1_ref, rank1_ref, gate1_ref, 2)

    z, y = tp // side, lax.rem(tp, side)
    cut = feats // 2
    low, high = pl.ds(0, cut), pl.ds(cut, cut)
    await_bytes(back0_ref.at[everything], osend.at[1])
    await_bytes(back0_ref.at[everything], osend.at[2])
    own = pltpu.make_async_copy(hid_ref, dst_ref.at[z, y], own_sem)
    own.start()
    own.wait()

    def push(ref, to_z, to_y, k):
        pltpu.make_async_remote_copy(ref, ref, gsend.at[k], grecv.at[k], device_id={'tp': to_z * side + to_y}, device_id_type=MESH).start()

    for j in range(1, side):
        push(dst_ref.at[z, y, low], z, lax.rem(y + j, side), 0)
        push(dst_ref.at[z, y, high], lax.rem(z + j, side), y, 1)
    some = pl.ds(0, side - 1)
    await_bytes(dst_ref.at[z, some, low], grecv.at[0])
    for j in range(1, side):
        push(dst_ref.at[z, :, low], lax.rem(z + j, side), y, 2)
    await_bytes(dst_ref.at[some, y, high], grecv.at[1])
    for j in range(1, side):
        push(dst_ref.at[:, y, high], z, lax.rem(y + j, side), 3)
    await_bytes(dst_ref.at[some, :, low], grecv.at[2])
    await_bytes(dst_ref.at[:, some, high], grecv.at[3])
    await_bytes(dst_ref.at[z, some, low], gsend.at[0])
    await_bytes(dst_ref.at[some, y, high], gsend.at[1])
    await_bytes(dst_ref.at[some, :, low], gsend.at[2])
    await_bytes(dst_ref.at[:, some, high], gsend.at[3])
    sent = pl.ds(0, all_slots - slots)
    for mat, ref in enumerate((newg_ref, newu_ref, newd_ref)):
        await_bytes(ref, mrecv.at[mat])
        await_bytes(held_ref.at[sent, mat], msend.at[mat])
    await_bytes(held_ref.at[sent], hsend)
    await_bytes(rows0_ref.at[pl.ds(0, group - 1)], rsend)
    own_slot = tp // slots == core
    for layer, (mine_ref, swap) in enumerate(((mine0_ref, swap0), (mine1_ref, swap1))):
        swap.wait_send()

        @pl.when(own_slot)
        def _():
            await_bytes(mine_ref.at[pl.ds(0, cols - 1)], wsend.at[layer])

        @pl.when(jnp.logical_not(own_slot))
        def _():
            await_bytes(mine_ref, wsend.at[layer])


def run_layers(source, holds, ids, gates, x, residual, halves, pieces, group, cols, cap):
    feats, tokens = residual.shape
    width = x.shape[1]
    side = int(round(cols ** 0.5))
    _, slots, _, part, _ = halves[0].shape
    depth = pieces[0].shape[3]
    all_slots = group * slots
    half = cap // 2
    ffn = 2 * cols * part

    def vmem(*shape, dtype=BF16):
        return pltpu.VMEM(shape, dtype)

    weights = vmem(cols, 3, part, width)
    blocks = vmem(group * cols, feats, half)
    rows = vmem(group, half, width)
    held = vmem(all_slots, 3, depth, width)
    return pl.pallas_call(
        functools.partial(layers_kernel, group, cols, side, cap),
        out_shape=(jax.ShapeDtypeStruct((side, side, feats, tokens), BF16),) + (jax.ShapeDtypeStruct(pieces[0].shape, BF16),) * 3,
        in_specs=[SMEM] + [VMEM] * 5 + [ANY] * 6,
        out_specs=(ANY,) * 4,
        scratch_shapes=[vmem(all_slots, tokens, dtype=jnp.int32), vmem(all_slots, tokens, dtype=F32)] * 2 + [rows, rows] + [weights] * 4
                       + [blocks, blocks, vmem(width, ffn), blocks, blocks, blocks, vmem(feats, tokens, dtype=F32), vmem(feats, tokens), held, held,
                          DMA, DMA, DMA((group // 2,)), DMA((2,)), DMA((2,)), DMA((2,)), DMA((2,)), DMA, DMA, DMA((3,)), DMA((3,)), DMA((3,)), DMA((3, group // 2)), DMA((4,)), DMA((4,))],
        compiler_params=pltpu.CompilerParams(has_side_effects=True, collective_id=0, vmem_limit_bytes=62 << 20),
    )(source, holds, ids, gates, x, residual, *halves, *pieces)


def solution(mesh):
    group = mesh.shape['ep']
    cols = mesh.shape['tp']
    row_spec = P(('rep', 'ep'), None)
    layer_spec = P(None, ('rep', 'ep'), None)
    col_spec = P(None, ('rep', 'ep'), None, 'tp')
    down_spec = P(None, ('rep', 'ep'), 'tp', None)
    map_spec = P(None, None)

    def device_step(x_in, route_ids, gate_vals, w_gate, w_up, w_down, old_map, move_src, move_dst):
        layers, slots, width, part = w_gate.shape
        tokens, top_k = route_ids.shape[1], route_ids.shape[2]
        all_slots = group * slots
        cap = 2 * tokens * top_k // all_slots
        half = cap // 2
        feats = width // cols
        ep = lax.axis_index('ep')
        tp = lax.axis_index('tp')

        slot_ids = jnp.arange(all_slots, dtype=jnp.int32)
        again = (old_map[:, :, None] == old_map[:, None, :]) & (slot_ids[None, :] < slot_ids[:, None])[None]
        holds = jnp.where(jnp.any(again, axis=2), -1, old_map)[:, :, None]

        pieces = group // layers
        mine = ep // pieces
        hit = slot_ids[:, None] == move_dst[mine][None, :]
        source = jnp.where(jnp.any(hit, axis=1), jnp.sum(jnp.where(hit, move_src[mine][None, :], 0), axis=1), slot_ids)

        residual = lax.dynamic_slice_in_dim(x_in, tp * feats, feats, axis=1).T
        mats = (jnp.swapaxes(w_gate, 2, 3), jnp.swapaxes(w_up, 2, 3), w_down)
        halves = [m.reshape(layers, slots, 2, part // 2, width) for m in mats]
        groups = [m.reshape(layers, slots, pieces, part // pieces, width) for m in mats]
        y_out, *new = run_layers(source, holds, jnp.swapaxes(route_ids, 1, 2), jnp.swapaxes(gate_vals, 1, 2), x_in, residual, halves, groups, group, cols, cap)
        y_out = y_out.reshape(width, tokens).T
        new = [m.reshape(layers, slots, part, width) for m in new]
        return y_out, jnp.swapaxes(new[0], 2, 3), jnp.swapaxes(new[1], 2, 3), new[2]

    return jax.shard_map(device_step, mesh=mesh, in_specs=(row_spec, layer_spec, layer_spec, col_spec, col_spec, down_spec, map_spec, map_spec, map_spec), out_specs=(row_spec, col_spec, col_spec, down_spec), check_vma=False)
```

```python
import functools

import jax
import jax.numpy as jnp
from jax import lax
from jax.experimental import pallas as pl
from jax.experimental.pallas import tpu as pltpu
from jax.sharding import PartitionSpec as P

EXPERTS = 40
F32 = jnp.float32
BF16 = jnp.bfloat16
VMEM = pl.BlockSpec(memory_space=pltpu.VMEM)
SMEM = pl.BlockSpec(memory_space=pltpu.SMEM)
ANY = pl.BlockSpec(memory_space=pl.ANY)
MESH = pl.DeviceIdType.MESH
DMA = pltpu.SemaphoreType.DMA


def params(collective):
    return pltpu.CompilerParams(has_side_effects=True, collective_id=collective)


def signal_all(group, cols):
    ep, tp = lax.axis_index('ep'), lax.axis_index('tp')
    barrier = pltpu.get_barrier_semaphore()

    def tell(k, carry):
        peer = {'tp': lax.rem(tp + k // group, cols), 'ep': lax.rem(ep + lax.rem(k, group), group)}
        pl.semaphore_signal(barrier, inc=1, device_id=peer, device_id_type=MESH)
        return carry

    lax.fori_loop(1, group * cols, tell, 0)


def wait_all(group, cols):
    pl.semaphore_wait(pltpu.get_barrier_semaphore(), group * cols - 1)


def post(src, dst, to_ep, to_tp, send_sem, recv_sem):
    ep, tp = lax.axis_index('ep'), lax.axis_index('tp')
    here = jnp.logical_and(to_ep == ep, to_tp == tp)

    @pl.when(jnp.logical_not(here))
    def _():
        pltpu.make_async_remote_copy(src, dst, send_sem, recv_sem, device_id={'tp': to_tp, 'ep': to_ep}, device_id_type=MESH).start()

    @pl.when(here)
    def _():
        pltpu.make_async_copy(src, dst, recv_sem).start()


def await_bytes(ref, sem):
    pltpu.make_async_copy(ref, ref, sem).wait()


def layers_kernel(group, cols, side, cap, source_ref, sexp_ref, ids_ref, gates_ref, x_ref, res_ref, g16, u16, d16, g8, u8, d8,
                  dst_ref, newg_ref, newu_ref, newd_ref, rank0_ref, gate0_ref, rank1_ref, gate1_ref, rsend_ref, rows0_ref, mine0_ref, other0_ref, mine1_ref, other1_ref,
                  out_ref, send_ref, down_ref, back0_ref, rows1_ref, back1_ref, acc_ref, hid_ref, held_ref, moves_ref,
                  own_sem, rsend, rrecv, wsend, wrecv, ssend, srecv, hsend, hrecv, msend, mrecv, osend, orecv, gsend, grecv):
    ep, tp = lax.axis_index('ep'), lax.axis_index('tp')
    me = ep * cols + tp
    core = lax.rem(ep, 2)
    here = ep // 2
    planes = group // 2
    width = mine0_ref.shape[3]
    ffn_half = mine0_ref.shape[0] * mine0_ref.shape[2]
    feats, half = out_ref.shape[1:]
    all_slots, tokens = rank0_ref.shape
    slots = all_slots // group
    pieces = group // 2
    signal_all(group, cols)
    def near(i):
        hop = jnp.where(i == 0, 1, jnp.where(i == 1, planes - 1, jnp.where(i == 2, 2, 0)))
        return lax.rem(here + hop, planes)

    def take_plane(ref, sem, i):
        plane = near(i)
        per = ref.shape[0] // planes
        await_bytes(ref.at[pl.ds(per * plane, per)], sem.at[plane])

    row_iota = lax.broadcasted_iota(jnp.int32, (cap, tokens), 0)

    def table(layer, rank_ref, gate_ref):
        holds = sexp_ref[layer]
        taken = jnp.zeros((all_slots, tokens), F32)
        gate = jnp.zeros((all_slots, tokens), F32)
        for j in range(ids_ref.shape[1]):
            match = ids_ref[layer, j:j + 1, :] == holds
            taken = jnp.where(match, 1.0, taken)
            gate = jnp.where(match, gates_ref[layer, j:j + 1, :], gate)
        earlier = lax.broadcasted_iota(jnp.int32, (tokens, tokens), 0) < lax.broadcasted_iota(jnp.int32, (tokens, tokens), 1)
        rank = jnp.dot(taken.astype(BF16), earlier.astype(BF16), preferred_element_type=F32).astype(jnp.int32)
        rank_ref[...] = jnp.where(taken > 0.0, rank, -1)
        gate_ref[...] = gate

    def first_rows(i, carry):
        pick = (rank0_ref[pl.ds(i * cols + tp, 1), :] == row_iota).astype(BF16)
        rows = jnp.dot(pick, x_ref[...], preferred_element_type=F32).astype(BF16)
        rsend_ref[2 * i] = rows[:half]
        rsend_ref[2 * i + 1] = rows[half:]
        return carry

    def send_weights(layer, mine_ref):
        def one(k, carry):
            slot = lax.rem(tp + k // 2, slots)
            part = lax.rem(k, 2)
            for mat, ref in enumerate((g16, u16, d16)):
                post(ref.at[layer, slot, part], mine_ref.at[tp, mat], ep - core + part, slots * core + slot, wsend.at[layer], wrecv.at[layer])
            return carry

        lax.fori_loop(0, 2 * slots, one, 0)

    def swap_weights(layer, mine_ref, other_ref):
        await_bytes(mine_ref, wrecv.at[layer])
        swap = pltpu.make_async_remote_copy(mine_ref, other_ref, ssend.at[layer], srecv.at[layer], device_id={'ep': ep + 1 - 2 * core}, device_id_type=MESH)
        swap.start()
        return swap

    def send_rows(k, carry):
        to = 2 * near(k // 2) + lax.rem(k, 2)
        post(rsend_ref.at[to], rows0_ref.at[ep], to, tp, rsend, rrecv.at[here])
        return carry

    def gather_moves(k, carry):
        to = 2 * near(k // 2) + lax.rem(k, 2)
        for mat, ref in enumerate((g8, u8, d8)):
            post(ref.at[to // pieces, :, lax.rem(to, pieces)], held_ref.at[pl.ds(ep * slots, slots), mat], to, tp, hsend, hrecv)
        return carry

    def permute(k, carry):
        moves_ref[k] = held_ref[source_ref[k]]
        return carry

    def send_moves(i, to_core):
        to = 2 * near(i) + to_core
        for mat, ref in enumerate((newg_ref, newu_ref, newd_ref)):
            post(moves_ref.at[pl.ds(to * slots, slots), mat], ref.at[ep // pieces, :, lax.rem(ep, pieces)], to, tp, msend.at[mat], mrecv.at[mat])

    def experts(wide, rows_ref, mine_ref, other_ref, dest_ref, stage):
        def whole(k):
            return jnp.concatenate([mine_ref[:, k].reshape(ffn_half, width), other_ref[:, k].reshape(ffn_half, width)], axis=0)

        def pair(i):
            return 2 * near(2 * (i // 2)) + lax.rem(i, 2), 2 * near(2 * (i // 2) + 1) + lax.rem(i, 2)

        def compute(i):
            one, two = pair(i)
            if wide:
                rows = jnp.concatenate([rows_ref[pl.ds(one * cols, cols)].reshape(width, half), rows_ref[pl.ds(two * cols, cols)].reshape(width, half)], axis=1)
            else:
                rows = jnp.concatenate([rows_ref[one], rows_ref[two]], axis=0)
            dims = (((1,), (0 if wide else 1,)), ((), ()))
            gate = lax.dot_general(whole(0), rows, dims, preferred_element_type=F32)
            up = lax.dot_general(whole(1), rows, dims, preferred_element_type=F32)
            act = (jax.nn.silu(gate) * up).astype(BF16)
            out = jnp.dot(down_ref[...], act, preferred_element_type=F32).astype(BF16)
            out_ref[pl.ds(one * cols, cols)] = out[:, :half].reshape(cols, feats, half)
            out_ref[pl.ds(two * cols, cols)] = out[:, half:].reshape(cols, feats, half)

        def send(i):
            one, two = pair(i)

            def each(k, carry):
                to_ep = jnp.where(lax.rem(k, 2) == 0, one, two)
                to_tp = lax.rem(tp + k // 2, cols)
                post(out_ref.at[to_ep * cols + to_tp], dest_ref.at[me], to_ep, to_tp, osend.at[stage], orecv.at[stage, here])
                return carry

            lax.fori_loop(0, 2 * cols, each, 0)

        down_ref[...] = whole(2).T
        arrived = orecv.at[1] if wide else rrecv
        take_plane(rows_ref, arrived, 0)
        take_plane(rows_ref, arrived, 1)
        compute(0)
        compute(1)
        send(0)
        take_plane(rows_ref, arrived, 2)
        take_plane(rows_ref, arrived, 3)
        compute(2)
        send(1)
        compute(3)
        send(2)
        send(3)

    def combine(back_ref, rank_ref, gate_ref, stage):
        for i in range(planes):
            take_plane(back_ref, orecv.at[stage], i)
            plane = near(i)

            def step(column, carry):
                block = 2 * plane * cols + column
                slot = plane * cols + column
                rows = jnp.concatenate([back_ref[block], back_ref[block + cols]], axis=1)
                pick = (rank_ref[pl.ds(slot, 1), :] == row_iota).astype(BF16)
                chosen = jnp.dot(rows, pick, preferred_element_type=F32)
                acc_ref[...] += gate_ref[pl.ds(slot, 1), :] * chosen
                return carry

            lax.fori_loop(0, cols, step, 0)
        hid_ref[...] = acc_ref[...].astype(BF16)

    everything = pl.ds(0, group * cols - 1)

    table(0, rank0_ref, gate0_ref)
    lax.fori_loop(0, planes, first_rows, 0)
    wait_all(group, cols)
    send_weights(0, mine0_ref)
    lax.fori_loop(0, group, send_rows, 0)
    send_weights(1, mine1_ref)
    table(1, rank1_ref, gate1_ref)
    acc_ref[...] = res_ref[...].astype(F32)
    swap0 = swap_weights(0, mine0_ref, other0_ref)
    swap0.wait_recv()
    experts(False, rows0_ref, mine0_ref, other0_ref, back0_ref, 0)
    lax.fori_loop(0, group, gather_moves, 0)
    swap1 = swap_weights(1, mine1_ref, other1_ref)
    combine(back0_ref, rank0_ref, gate0_ref, 0)
    await_bytes(back0_ref.at[everything], osend.at[0])

    def place(i):
        plane = near(2 * (i // (2 * cols)) + lax.rem(i, 2))
        return plane, lax.rem(tp + lax.rem(i, 2 * cols) // 2, cols)

    def choose(i):
        plane, column = place(i)
        pick = (rank1_ref[pl.ds(plane * cols + column, 1), :] == row_iota).astype(BF16)
        rows = lax.dot_general(hid_ref[...], pick, (((1,), (1,)), ((), ())), preferred_element_type=F32).astype(BF16)
        block = 2 * plane * cols + column
        send_ref[block] = rows[:, :half]
        send_ref[block + cols] = rows[:, half:]

    def ship(i):
        plane, column = place(i)
        block = 2 * plane * cols + column
        post(send_ref.at[block], rows1_ref.at[me], 2 * plane, column, osend.at[1], orecv.at[1, here])
        post(send_ref.at[block + cols], rows1_ref.at[me], 2 * plane + 1, column, osend.at[1], orecv.at[1, here])

    choose(0)

    def step(i, carry):
        choose(i)
        ship(i - 1)
        return carry

    lax.fori_loop(1, all_slots, step, 0)
    swap1.wait_recv()
    ship(all_slots - 1)
    await_bytes(held_ref, hrecv)
    lax.fori_loop(0, all_slots, permute, 0)
    acc_ref[...] = hid_ref[...].astype(F32)
    experts(True, rows1_ref, mine1_ref, other1_ref, back1_ref, 2)
    for to_core in range(2):
        for i in range(planes):
            send_moves(i, to_core)
    combine(back1_ref, rank1_ref, gate1_ref, 2)

    z, y = tp // side, lax.rem(tp, side)
    cut = feats // 2
    low, high = pl.ds(0, cut), pl.ds(cut, cut)
    await_bytes(back0_ref.at[everything], osend.at[1])
    await_bytes(back0_ref.at[everything], osend.at[2])
    own = pltpu.make_async_copy(hid_ref, dst_ref.at[z, y], own_sem)
    own.start()
    own.wait()

    def push(ref, to_z, to_y, k):
        pltpu.make_async_remote_copy(ref, ref, gsend.at[k], grecv.at[k], device_id={'tp': to_z * side + to_y}, device_id_type=MESH).start()

    for j in range(1, side):
        push(dst_ref.at[z, y, low], z, lax.rem(y + j, side), 0)
        push(dst_ref.at[z, y, high], lax.rem(z + j, side), y, 1)
    some = pl.ds(0, side - 1)
    await_bytes(dst_ref.at[z, some, low], grecv.at[0])
    for j in range(1, side):
        push(dst_ref.at[z, :, low], lax.rem(z + j, side), y, 2)
    await_bytes(dst_ref.at[some, y, high], grecv.at[1])
    for j in range(1, side):
        push(dst_ref.at[:, y, high], z, lax.rem(y + j, side), 3)
    await_bytes(dst_ref.at[some, :, low], grecv.at[2])
    await_bytes(dst_ref.at[:, some, high], grecv.at[3])
    await_bytes(dst_ref.at[z, some, low], gsend.at[0])
    await_bytes(dst_ref.at[some, y, high], gsend.at[1])
    await_bytes(dst_ref.at[some, :, low], gsend.at[2])
    await_bytes(dst_ref.at[:, some, high], gsend.at[3])
    sent = pl.ds(0, all_slots - slots)
    for mat, ref in enumerate((newg_ref, newu_ref, newd_ref)):
        await_bytes(ref, mrecv.at[mat])
        await_bytes(held_ref.at[sent, mat], msend.at[mat])
    await_bytes(held_ref.at[sent], hsend)
    await_bytes(rows0_ref.at[pl.ds(0, group - 1)], rsend)
    own_slot = tp // slots == core
    for layer, (mine_ref, swap) in enumerate(((mine0_ref, swap0), (mine1_ref, swap1))):
        swap.wait_send()

        @pl.when(own_slot)
        def _():
            await_bytes(mine_ref.at[pl.ds(0, cols - 1)], wsend.at[layer])

        @pl.when(jnp.logical_not(own_slot))
        def _():
            await_bytes(mine_ref, wsend.at[layer])


def run_layers(source, holds, ids, gates, x, residual, halves, pieces, group, cols, cap):
    feats, tokens = residual.shape
    width = x.shape[1]
    side = int(round(cols ** 0.5))
    _, slots, _, part, _ = halves[0].shape
    depth = pieces[0].shape[3]
    all_slots = group * slots
    half = cap // 2
    ffn = 2 * cols * part

    def vmem(*shape, dtype=BF16):
        return pltpu.VMEM(shape, dtype)

    weights = vmem(cols, 3, part, width)
    blocks = vmem(group * cols, feats, half)
    rows = vmem(group, half, width)
    held = vmem(all_slots, 3, depth, width)
    return pl.pallas_call(
        functools.partial(layers_kernel, group, cols, side, cap),
        out_shape=(jax.ShapeDtypeStruct((side, side, feats, tokens), BF16),) + (jax.ShapeDtypeStruct(pieces[0].shape, BF16),) * 3,
        in_specs=[SMEM] + [VMEM] * 5 + [ANY] * 6,
        out_specs=(ANY,) * 4,
        scratch_shapes=[vmem(all_slots, tokens, dtype=jnp.int32), vmem(all_slots, tokens, dtype=F32)] * 2 + [rows, rows] + [weights] * 4
                       + [blocks, blocks, vmem(width, ffn), blocks, blocks, blocks, vmem(feats, tokens, dtype=F32), vmem(feats, tokens), held, held,
                          DMA, DMA, DMA((group // 2,)), DMA((2,)), DMA((2,)), DMA((2,)), DMA((2,)), DMA, DMA, DMA((3,)), DMA((3,)), DMA((3,)), DMA((3, group // 2)), DMA((4,)), DMA((4,))],
        compiler_params=pltpu.CompilerParams(has_side_effects=True, collective_id=0, vmem_limit_bytes=62 << 20),
    )(source, holds, ids, gates, x, residual, *halves, *pieces)


def solution(mesh):
    group = mesh.shape['ep']
    cols = mesh.shape['tp']
    row_spec = P(('rep', 'ep'), None)
    layer_spec = P(None, ('rep', 'ep'), None)
    col_spec = P(None, ('rep', 'ep'), None, 'tp')
    down_spec = P(None, ('rep', 'ep'), 'tp', None)
    map_spec = P(None, None)

    def device_step(x_in, route_ids, gate_vals, w_gate, w_up, w_down, old_map, move_src, move_dst):
        layers, slots, width, part = w_gate.shape
        tokens, top_k = route_ids.shape[1], route_ids.shape[2]
        all_slots = group * slots
        cap = 2 * tokens * top_k // all_slots
        half = cap // 2
        feats = width // cols
        ep = lax.axis_index('ep')
        tp = lax.axis_index('tp')

        slot_ids = jnp.arange(all_slots, dtype=jnp.int32)
        again = (old_map[:, :, None] == old_map[:, None, :]) & (slot_ids[None, :] < slot_ids[:, None])[None]
        holds = jnp.where(jnp.any(again, axis=2), -1, old_map)[:, :, None]

        pieces = group // layers
        mine = ep // pieces
        hit = slot_ids[:, None] == move_dst[mine][None, :]
        source = jnp.where(jnp.any(hit, axis=1), jnp.sum(jnp.where(hit, move_src[mine][None, :], 0), axis=1), slot_ids)

        residual = lax.dynamic_slice_in_dim(x_in, tp * feats, feats, axis=1).T
        mats = (jnp.swapaxes(w_gate, 2, 3), jnp.swapaxes(w_up, 2, 3), w_down)
        halves = [m.reshape(layers, slots, 2, part // 2, width) for m in mats]
        groups = [m.reshape(layers, slots, pieces, part // pieces, width) for m in mats]
        y_out, *new = run_layers(source, holds, jnp.swapaxes(route_ids, 1, 2), jnp.swapaxes(gate_vals, 1, 2), x_in, residual, halves, groups, group, cols, cap)
        y_out = y_out.reshape(width, tokens).T
        new = [m.reshape(layers, slots, part, width) for m in new]
        return y_out, jnp.swapaxes(new[0], 2, 3), jnp.swapaxes(new[1], 2, 3), new[2]

    return jax.shard_map(device_step, mesh=mesh, in_specs=(row_spec, layer_spec, layer_spec, col_spec, col_spec, down_spec, map_spec, map_spec, map_spec), out_specs=(row_spec, col_spec, col_spec, down_spec), check_vma=False)
```
